128 devices in a mesh: grp: 4 (over z), dev: 32 (over x, y, core).
Axes of the slice: x: 4, y: 4, z: 4, core: 2. Of those that a mesh axis runs over, the one named last changes fastest.
Arguments:
- matrix_tiles: bfloat16 [10240, 128, 1024], P(('grp', 'dev')), may hold values from -0.125 to 0.125
- tile_column: int32 [10240], P(('grp', 'dev')), may hold values from 0 to 255
- block_counts: int32 [4096], P(('grp', 'dev')), may hold values from 1 to 4, as said below
- destination: int32 [4096], P(('grp', 'dev')), may hold values from 0 to 31, as said below
- row_bounds: bfloat16 [524288], P(('grp', 'dev')), may hold values from -6 to 6
- dual_start: bfloat16 [524288], P(('grp', 'dev')), may hold values from 0 to 1
- primal_start: float32 [262144], replicated, may hold values from 0 to 0.5
- cost_vector: float32 [262144], replicated, may hold values from -6 to 6
- upper_bound: float32 [262144], replicated, may hold values from 0.5 to 2
Outputs:
- primal_final: float32 [262144], replicated
- dual_final: float32 [524288], P(('grp', 'dev'))
- weight_final: float32 [1], replicated
The draws below stay inside these ranges and needn't reach their ends.
Inputs may be any that keep to these rules, and one draw needn't show every extreme that they name: `block_counts`: each device's 32 row blocks have 1 to 4 tiles each and 80 at most together; some device has exactly 80 in every draw. `destination`: on every device the 32 entries are each of 0 to 31 once.
All inputs are finite; a program needn't handle non-finite values.
Results may differ from the reference program's by a relative error of at most 0.0015.
Values may be sent and summed in bfloat16 or wider, within the bound.
No kernel may reach another device: no remote copies, remote signals or barrier semaphores. Data moves between devices by JAX's collectives and lax.ppermute only.
A program may use at most 128 MiB of HBM per device.

```python
import jax
import jax.numpy as jnp
from jax import lax

CB = 1024
NCB = 256
TR = 128
MAXC = 4
ITERS = 3
RB_DEV = 32
POOL_DEV = 80
RBLK = 4096
ROWS = 524288
COLS = 262144
N_GRP = 4
N_DEV = 32


def layout_pair(key):
    device_count = RBLK // RB_DEV
    base_key = jax.random.fold_in(key, 7)
    key_extra, key_heavy, key_rank, key_tie = jax.random.split(base_key, 4)
    extra_tiles = jax.random.randint(key_extra, (device_count,), 0, POOL_DEV - RB_DEV + 1)
    heaviest = jax.random.randint(key_heavy, (), 0, device_count)
    extra_tiles = jnp.where(jnp.arange(device_count) == heaviest, POOL_DEV - RB_DEV, extra_tiles)
    rank_of = jax.vmap(lambda sub: jax.random.permutation(sub, RB_DEV))(jax.random.split(key_rank, device_count))
    counts = 1 + jnp.clip(extra_tiles[:, None] - rank_of * (MAXC - 1), 0, MAXC - 1)
    tie_break = jax.vmap(lambda sub: jax.random.permutation(sub, RB_DEV))(jax.random.split(key_tie, device_count))
    sorted_slots = jnp.argsort(counts * RB_DEV + tie_break, axis=1)
    position = jnp.argsort(sorted_slots, axis=1)
    member = (jnp.arange(device_count) % RB_DEV)[:, None]
    target_dev = (position + member) % RB_DEV
    return (counts.astype(jnp.int32).reshape(RBLK), target_dev.astype(jnp.int32).reshape(RBLK))


def draw_block_counts(key, part):
    return layout_pair(key)[0]


def draw_destination(key, part):
    return layout_pair(key)[1]


def plant(result, rng, low, top_value):
    longest = result.shape.index(max(result.shape))
    spots = []
    for shift in (0, 1):
        where = [jax.random.randint(jax.random.fold_in(rng, axis), (), 0, length) for axis, length in enumerate(result.shape)]
        where[longest] = (where[longest] + shift) % result.shape[longest]
        spots.append(tuple(where))
    return result.at[spots[0]].set(low).at[spots[1]].set(top_value)


def steps_of(own_key, extent, shards, low, top_value):
    level = 1.0
    for dim, blocks in shards:
        heights = jax.random.uniform(jax.random.fold_in(jax.random.fold_in(own_key, 6), dim), (blocks,), jnp.float32, low / len(shards), top_value / len(shards))
        level = level * jnp.repeat(jnp.exp(heights), extent[dim] // blocks).reshape((-1,) + (1,) * (len(extent) - 1 - dim))
    return level


def bell_draw(own_key, shape, spread, reach, cuts=(), kind=jnp.bfloat16):
    gain = steps_of(own_key, shape, cuts, -0.22, 0.18) if cuts else 1.0
    drawn = jax.random.normal(own_key, shape, jnp.float32) * spread * gain
    return jnp.minimum(jnp.maximum(drawn, -reach), reach).astype(kind)


def setup_inputs(seed: int = 0) -> dict:
    key_list = jax.random.split(jax.random.key(seed), 10)
    matrix_tiles = bell_draw(key_list[0], (N_GRP * N_DEV * POOL_DEV, TR, CB), (2 * CB) ** -0.5, 0.125, ((0, 128),))
    tile_column = plant(jax.random.randint(key_list[1], (N_GRP * N_DEV * POOL_DEV,), 0, NCB), jax.random.fold_in(key_list[1], 1), 0, NCB - 1).astype(jnp.int32)
    block_counts = draw_block_counts(jax.random.fold_in(key_list[9], 71), 0)
    destination = draw_destination(jax.random.fold_in(key_list[9], 71), 0)
    row_bounds = bell_draw(key_list[4], (ROWS,), 1.0, 6.0, ((0, 128),))
    dual_start = jnp.clip(1.0 * jax.random.uniform(key_list[5], (ROWS,), jnp.float32) ** steps_of(key_list[5], (ROWS,), ((0, 128),), -0.2, 0.2), 0.0, 1.0).astype(jnp.bfloat16)
    primal_start = jnp.clip(jax.random.uniform(key_list[6], (COLS,), jnp.float32, 0.0, 0.5), 0.0, 0.5)
    cost_vector = bell_draw(key_list[7], (COLS,), 1.0, 6.0, (), jnp.float32)
    upper_bound = jnp.clip(jax.random.uniform(key_list[8], (COLS,), jnp.float32, 0.5, 2.0), 0.5, 2.0)
    return {"matrix_tiles": matrix_tiles, "tile_column": tile_column, "block_counts": block_counts, "destination": destination, "row_bounds": row_bounds, "dual_start": dual_start, "primal_start": primal_start, "cost_vector": cost_vector, "upper_bound": upper_bound}


step_scale = 0.3

def reference(matrix_tiles, tile_column, block_counts, destination, row_bounds, dual_start, primal_start, cost_vector, upper_bound):
    device_count = N_GRP * N_DEV
    tile_set = matrix_tiles.reshape(device_count, POOL_DEV, TR, CB)
    tile_cols = tile_column.reshape(device_count, POOL_DEV)
    counts = block_counts.reshape(device_count, RB_DEV)
    starts = jnp.cumsum(counts, axis=1) - counts
    slot_ids = jnp.arange(POOL_DEV, dtype=jnp.int32)
    owners = lax.optimization_barrier(jnp.sum((starts[:, None, 1:] <= slot_ids[None, :, None]).astype(jnp.int32), axis=2))
    is_live = slot_ids[None, :] < lax.optimization_barrier(jnp.sum(counts, axis=1))[:, None]

    def apply_rows(vector_bf):
        vector_table = vector_bf.astype(jnp.float32).reshape(NCB, CB)

        def per_device(entries):
            tile_d, col_d, own_d, live_d = entries
            product = jnp.einsum('src,sc->sr', tile_d.astype(jnp.float32), vector_table[col_d], precision=lax.Precision.HIGHEST)
            product = jnp.where(live_d[:, None], product, 0.0)
            return jax.ops.segment_sum(product, own_d, num_segments=RB_DEV)
        return lax.map(per_device, (tile_set, tile_cols, owners, is_live))

    def apply_columns(rows_bf):

        def per_device(accum, entries):
            tile_d, col_d, own_d, live_d, rows_d = entries
            product = jnp.einsum('src,sr->sc', tile_d.astype(jnp.float32), rows_d.astype(jnp.float32)[own_d], precision=lax.Precision.HIGHEST)
            product = jnp.where(live_d[:, None], product, 0.0)
            return (accum + jax.ops.segment_sum(product, col_d, num_segments=NCB), None)
        accum, unused = lax.scan(per_device, jnp.zeros((NCB, CB), jnp.float32), (tile_set, tile_cols, owners, is_live, rows_bf))
        return accum.reshape(-1)
    bounds = row_bounds.astype(jnp.float32).reshape(device_count, RB_DEV, TR)
    dual_state = dual_start.astype(jnp.float32).reshape(device_count, RB_DEV, TR)
    primal = primal_start
    weight = jnp.ones((), jnp.float32)
    row_image = apply_rows(primal.astype(jnp.bfloat16))
    for iteration in range(ITERS):
        step_primal = step_scale / weight
        step_dual = step_scale * weight
        gradient = apply_columns(dual_state.astype(jnp.bfloat16))
        primal_next = jnp.clip(primal - step_primal * (cost_vector - gradient), 0.0, upper_bound)
        change = jnp.sum((primal_next - primal) ** 2)
        next_image = apply_rows(primal_next.astype(jnp.bfloat16))
        dual_state = jnp.maximum(dual_state + step_dual * (bounds - (2.0 * next_image - row_image)), 0.0)
        violation = jnp.sum(jnp.maximum(bounds - next_image, 0.0) ** 2)
        weight = jnp.sqrt(weight * jnp.sqrt((violation + 1e-06) / (change + 1e-06)))
        primal = primal_next
        row_image = next_image
    grouped = dual_state.reshape(N_GRP, N_DEV, RB_DEV, TR)
    target = destination.reshape(N_GRP, N_DEV, RB_DEV)
    group_index = jnp.broadcast_to(jnp.arange(N_GRP, dtype=jnp.int32)[:, None, None], target.shape)
    member_index = jnp.broadcast_to(jnp.arange(N_DEV, dtype=jnp.int32)[None, :, None], target.shape)
    placed = jnp.zeros((N_GRP, N_DEV, N_DEV, TR), jnp.float32).at[group_index, target, member_index].set(grouped)
    return (primal, placed.reshape(-1), jnp.reshape(weight, (1,)))
```

```python
import jax
import jax.numpy as jnp
from jax import lax
from jax.experimental import pallas as pl
from jax.experimental.pallas import tpu as pltpu
from jax.sharding import Mesh
from jax.sharding import PartitionSpec as P

ITERS = 3
STEP = 0.3
TINY = 1e-06
BLOCKS = 32
SLOTS = 80
TR = 128
CB = 1024
COL_BLOCKS = 256
ROWS_P = 2048
CHIPS = 64
SHARE = 16
DMA_TILES = 8
UNROLL = 8

CHIP = ("grp", "dev_0", "dev_1")
CORE = "dev_2"
ALL = ("grp", "dev_0", "dev_1", "dev_2")
SWAP = [(0, 1), (1, 0)]
MIB = 1 << 20

f32 = jnp.float32
bf16 = jnp.bfloat16


def round_bf16(x):
    return x.astype(bf16).astype(f32)


def row_phase(count_ref, column_ref, tile_ref, table_ref, acc_ref, owner_ref, image_ref, arrive):
    def clear(s, carry):
        owner_ref[s] = BLOCKS
        return carry

    lax.fori_loop(0, SLOTS, clear, 0)

    def block(b, start):
        stop = start + count_ref[b]

        def tile(s, acc):
            arrive(s)
            owner_ref[s] = b
            col = column_ref[s]
            entries = [
                jnp.broadcast_to(table_ref[col, pl.ds(part, 1), :], (8, 128)) for part in range(8)
            ]
            out = []
            for g in range(TR // 8):
                rows = tile_ref[s, pl.ds(8 * g, 8), :].astype(f32)
                a = acc[g]
                for part in range(8):
                    a = a + rows[:, 128 * part : 128 * part + 128] * entries[part]
                out.append(a)
            return tuple(out)

        zero = tuple(jnp.zeros((8, 128), f32) for _ in range(TR // 8))
        acc = lax.fori_loop(start, stop, tile, zero)
        for g in range(TR // 8):
            acc_ref[b, pl.ds(8 * g, 8), :] = acc[g]
        return stop

    total = lax.fori_loop(0, BLOCKS, block, 0)

    def reduce_block(i, carry):
        for u in range(4):
            b = i * 4 + u
            image_ref[pl.ds(b, 1), :] = jnp.sum(acc_ref[b].T, axis=0, keepdims=True)
        return carry

    lax.fori_loop(0, BLOCKS // 4, reduce_block, 0)
    return total


def spread_rows(dual, spread_ref):
    for b in range(BLOCKS):
        spread_ref[b] = jnp.broadcast_to(dual[b : b + 1, :], (16, TR)).astype(bf16)
    spread_ref[BLOCKS] = jnp.zeros((16, TR), bf16)


def column_phase(column_ref, tile_ref, spread_ref, owner_ref, core, share_ref, rows):
    def clear(i, carry):
        for h in range(2):
            share_ref[h, i, pl.ds(0, SHARE), :] = jnp.zeros((SHARE, 128), f32)
        return carry

    lax.fori_loop(0, CHIPS, clear, 0)
    sub = lax.broadcasted_iota(jnp.int32, (8, 128), 0)

    def step(i, carry):
        results = []
        for u in range(UNROLL):
            s = i * UNROLL + u
            out = jnp.dot(
                spread_ref[owner_ref[s]], tile_ref[s], preferred_element_type=f32
            )
            r = out[0:8, 0:128]
            for part in range(1, 8):
                r = jnp.where(sub == part, out[0:8, 128 * part : 128 * part + 128], r)
            results.append(r)
        for u in range(UNROLL):
            col = column_ref[i * UNROLL + u]
            side = jnp.bitwise_xor(jnp.right_shift(col, 7), core)
            chunk = jnp.bitwise_and(jnp.right_shift(col, 1), CHIPS - 1)
            row = pl.multiple_of(jnp.bitwise_and(col, 1) * 8, 8)
            share_ref[side, chunk, pl.ds(row, 8), :] += results[u]
        return carry

    lax.fori_loop(0, SLOTS // UNROLL, step, 0)


def first_kernel(
    count_ref, column_ref, place_ref, tiles_hbm, table_in, dual_in, primal_hbm, cost_hbm, upper_hbm,
    tile_ref, image_ref, share_ref, primal_ref, cost_ref, upper_ref,
    table_ref, acc_ref, spread_ref, owner_ref, tile_sem, slice_sem,
):
    copies = [
        pltpu.make_async_copy(
            tiles_hbm.at[pl.ds(i * DMA_TILES, DMA_TILES)],
            tile_ref.at[pl.ds(i * DMA_TILES, DMA_TILES)],
            tile_sem.at[i],
        )
        for i in range(SLOTS // DMA_TILES)
    ]
    for c in copies:
        c.start()
    start = pl.multiple_of(place_ref[1] * SHARE, SHARE)
    slices = [
        pltpu.make_async_copy(src.at[pl.ds(start, SHARE)], dst, slice_sem.at[i])
        for i, (src, dst) in enumerate(
            ((primal_hbm, primal_ref), (cost_hbm, cost_ref), (upper_hbm, upper_ref))
        )
    ]
    for c in slices:
        c.start()

    def fill(i, carry):
        table_ref[pl.ds(i * 8, 8)] = round_bf16(table_in[pl.ds(i * 8, 8)])
        return carry

    lax.fori_loop(0, COL_BLOCKS // 8, fill, 0)

    def arrive(s):
        for i in range(SLOTS // DMA_TILES):

            @pl.when(s == i * DMA_TILES)
            def _():
                copies[i].wait()

    total = row_phase(
        count_ref, column_ref, tile_ref, table_ref, acc_ref, owner_ref, image_ref, arrive
    )
    for i in range(SLOTS // DMA_TILES):

        @pl.when(i * DMA_TILES >= total)
        def _():
            copies[i].wait()

    spread_rows(dual_in[...].astype(f32), spread_ref)
    column_phase(column_ref, tile_ref, spread_ref, owner_ref, place_ref[0], share_ref, SHARE)
    for c in slices:
        c.wait()


def fill_table(own_ref, other_ref, core, table_ref):
    def fill(i, carry):
        for ref, side in ((own_ref, core), (other_ref, 1 - core)):
            part = ref[i].astype(f32) if ref.dtype == bf16 else round_bf16(ref[i])
            at = side * (COL_BLOCKS // 2) + 2 * i
            table_ref[at] = part[0:8]
            table_ref[at + 1] = part[8:16]
        return carry

    lax.fori_loop(0, CHIPS, fill, 0)


def dual_step(bounds_ref, dual_in, image_in, image_ref, change_in, sigma):
    bounds = bounds_ref[...].astype(f32)
    image = image_ref[...]
    dual = jnp.maximum(
        dual_in[...].astype(f32) + sigma * (bounds - (2.0 * image - image_in[...])), 0.0
    )
    short = jnp.maximum(bounds - image, 0.0)
    violation = jnp.sum(short * short)
    lane = lax.broadcasted_iota(jnp.int32, (8, 128), 1)
    scalars = jnp.where(lane == 0, violation, jnp.where(lane == 1, change_in[...], 0.0))
    return dual, scalars


def middle_kernel(
    count_ref, column_ref, place_ref, tile_ref, own_ref, other_ref, bounds_ref, dual_in, image_in,
    change_in, sigma_in,
    dual_ref, image_ref, share_ref,
    table_ref, acc_ref, spread_ref, owner_ref,
):
    core = place_ref[0]
    fill_table(own_ref, other_ref, core, table_ref)
    row_phase(
        count_ref, column_ref, tile_ref, table_ref, acc_ref, owner_ref, image_ref, lambda s: None
    )
    dual, scalars = dual_step(
        bounds_ref, dual_in, image_in, image_ref, change_in, sigma_in[0:1, :]
    )
    dual_ref[...] = dual
    spread_rows(dual, spread_ref)

    def put(i, carry):
        for h in range(2):
            share_ref[h, i, pl.ds(SHARE, 8), :] = scalars
        return carry

    lax.fori_loop(0, CHIPS, put, 0)
    column_phase(column_ref, tile_ref, spread_ref, owner_ref, core, share_ref, SHARE + 8)


def last_kernel(
    count_ref, column_ref, place_ref, target_ref, tile_ref, own_ref, other_ref, bounds_ref, dual_in,
    image_in, change_in, sigma_in,
    primal_ref, send_ref,
    table_ref, acc_ref, owner_ref, image_ref,
):
    core = place_ref[0]
    fill_table(own_ref, other_ref, core, table_ref)

    def lay(i, carry):
        for ref, side in ((own_ref, core), (other_ref, 1 - core)):
            at = pl.multiple_of((side * CHIPS + i) * SHARE, SHARE)
            primal_ref[pl.ds(at, SHARE), :] = ref[i]
        return carry

    lax.fori_loop(0, CHIPS, lay, 0)
    row_phase(
        count_ref, column_ref, tile_ref, table_ref, acc_ref, owner_ref, image_ref, lambda s: None
    )
    dual, scalars = dual_step(
        bounds_ref, dual_in, image_in, image_ref, change_in, sigma_in[0:1, :]
    )

    def put(i, carry):
        send_ref[i] = scalars
        return carry

    lax.fori_loop(0, 4 * BLOCKS, put, 0)
    sub = lax.broadcasted_iota(jnp.int32, (8, 128), 0)
    first = place_ref[2] * BLOCKS
    for b in range(BLOCKS):
        send_ref[first + target_ref[b]] = jnp.where(
            sub == 0, jnp.broadcast_to(dual[b : b + 1, :], (8, 128)), scalars
        )


def next_weight(weight, scalars):
    lane = lax.broadcasted_iota(jnp.int32, (8, 128), 1)
    violation = jnp.sum(jnp.where(lane == 0, scalars, 0.0), axis=1, keepdims=True)
    change = jnp.sum(jnp.where(lane == 1, scalars, 0.0), axis=1, keepdims=True)
    ratio = jnp.broadcast_to((violation + TINY) / (change + TINY), (8, 128))
    return jnp.sqrt(weight * jnp.sqrt(ratio))


def update_kernel(
    arrived_ref, primal_in, cost_ref, upper_ref, weight_in,
    primal_ref, send_ref, change_ref, weight_ref, sigma_ref,
):
    rows = arrived_ref.shape[1]

    def add(i, total):
        return total + arrived_ref[i]

    total = lax.fori_loop(0, CHIPS, add, jnp.zeros((rows, 128), f32), unroll=8)
    weight = weight_in[...]
    if rows > SHARE:
        weight = next_weight(weight, total[SHARE:, :])
    tau = STEP / weight[0:1, :]
    primal = primal_in[...]
    new = jnp.clip(primal - tau * (cost_ref[...] - total[:SHARE, :]), 0.0, upper_ref[...])
    primal_ref[...] = new
    moved = new - primal
    change_ref[...] = jnp.full((8, 128), jnp.sum(moved * moved), f32)
    weight_ref[...] = weight
    sigma_ref[...] = STEP * weight
    out = new.astype(send_ref.dtype)

    def put(i, carry):
        send_ref[i] = out
        return carry

    lax.fori_loop(0, CHIPS, put, 0, unroll=8)


def finish_kernel(place_ref, arrived_ref, weight_in, dual_ref, weight_ref):
    def add(i, total):
        return total + arrived_ref[i]

    total = lax.fori_loop(0, 4 * BLOCKS, add, jnp.zeros((8, 128), f32), unroll=8)
    total = jnp.broadcast_to(total[1:2, :], (8, 128))
    weight_ref[...] = next_weight(weight_in[...], total)
    first = place_ref[2] * BLOCKS
    for b in range(BLOCKS):
        dual_ref[pl.ds(b, 1), :] = arrived_ref[first + b, pl.ds(0, 1), :]


SMEM = pl.BlockSpec(memory_space=pltpu.SMEM)
VMEM = pl.BlockSpec(memory_space=pltpu.VMEM)
ANY = pl.BlockSpec(memory_space=pl.ANY)


def sds(shape, dtype=f32):
    return jax.ShapeDtypeStruct(shape, dtype)


def call(kernel, name, in_specs, out_shape, out_specs, scratch=(), limit=24):
    return pl.pallas_call(
        kernel,
        name=name,
        in_specs=in_specs,
        out_specs=out_specs,
        out_shape=out_shape,
        scratch_shapes=list(scratch),
        compiler_params=pltpu.CompilerParams(vmem_limit_bytes=limit * MIB),
    )


TABLE = pltpu.VMEM((COL_BLOCKS, 8, 128), f32)
ACC = pltpu.VMEM((BLOCKS, TR, 128), f32)
SPREAD = pltpu.VMEM((BLOCKS + 1, 16, TR), bf16)
OWNER = pltpu.SMEM((SLOTS,), jnp.int32)
TILES = (SLOTS, TR, CB)


def both_sides(share):
    other = lax.ppermute(share[1], CORE, SWAP)
    return lax.all_to_all(share[0] + other, CHIP, 0, 0, tiled=True)


def gathered(send):
    own = lax.all_to_all(send, CHIP, 0, 0, tiled=True)
    return own, lax.ppermute(own, CORE, SWAP)


def per_device(
    matrix_tiles,
    tile_column,
    block_counts,
    destination,
    row_bounds,
    dual_start,
    primal_start,
    cost_vector,
    upper_bound,
):
    core = lax.axis_index(CORE)
    place = jnp.stack(
        [core, core * CHIPS + lax.axis_index(CHIP), lax.axis_index("grp")]
    ).astype(jnp.int32)
    bounds = row_bounds.reshape(BLOCKS, TR)
    dual = dual_start.reshape(BLOCKS, TR)
    wide = (ROWS_P, 128)

    tiles, image, share, primal, cost, upper = call(
        first_kernel,
        "first_pass",
        [SMEM, SMEM, SMEM, ANY, VMEM, VMEM, ANY, ANY, ANY],
        (
            pltpu.VMEM(TILES, bf16),
            sds((BLOCKS, TR)),
            sds((2, CHIPS, SHARE, 128)),
            sds((SHARE, 128)),
            sds((SHARE, 128)),
            sds((SHARE, 128)),
        ),
        (VMEM,) * 6,
        (TABLE, ACC, SPREAD, OWNER, pltpu.SemaphoreType.DMA((SLOTS // DMA_TILES,)),
         pltpu.SemaphoreType.DMA((3,))),
    )(
        block_counts, tile_column, place, matrix_tiles,
        primal_start.reshape(COL_BLOCKS, 8, 128), dual,
        primal_start.reshape(wide), cost_vector.reshape(wide), upper_bound.reshape(wide),
    )

    weight = jnp.ones((8, 128), f32)
    for iteration in range(ITERS):
        last = iteration == ITERS - 1
        arrived = both_sides(share)
        primal, send, change, weight, sigma = call(
            update_kernel,
            "update",
            [VMEM] * 5,
            (
                sds((SHARE, 128)),
                sds((CHIPS, SHARE, 128), f32 if last else bf16),
                sds((8, 128)),
                sds((8, 128)),
                sds((8, 128)),
            ),
            (VMEM,) * 5,
            limit=8,
        )(arrived, primal, cost, upper, weight)
        own, other = gathered(send)
        if not last:
            dual, image, share = call(
                middle_kernel,
                "middle_pass",
                [SMEM] * 3 + [VMEM] * 8,
                (sds((BLOCKS, TR)), sds((BLOCKS, TR)), sds((2, CHIPS, SHARE + 8, 128))),
                (VMEM,) * 3,
                (TABLE, ACC, SPREAD, OWNER),
            )(block_counts, tile_column, place, tiles, own, other, bounds, dual, image, change, sigma)
    primal_final, send = call(
        last_kernel,
        "last_pass",
        [SMEM] * 4 + [VMEM] * 8,
        (sds(wide), sds((4 * BLOCKS, 8, 128))),
        (VMEM,) * 2,
        (TABLE, ACC, OWNER, pltpu.VMEM((BLOCKS, TR), f32)),
    )(
        block_counts, tile_column, place, destination, tiles, own, other, bounds, dual, image,
        change, sigma,
    )
    arrived = lax.all_to_all(send, ALL, 0, 0, tiled=True)
    dual_final, weight = call(
        finish_kernel,
        "finish",
        [SMEM, VMEM, VMEM],
        (sds((BLOCKS, TR)), sds((8, 128))),
        (VMEM, VMEM),
        limit=8,
    )(place, arrived, weight)
    return (primal_final.reshape(-1), dual_final.reshape(-1), weight[0, 0:1])


def solution(mesh):
    split = Mesh(
        mesh.devices.reshape(mesh.shape["grp"], 4, 4, 2), ("grp", "dev_0", "dev_1", "dev_2")
    )
    return jax.shard_map(
        per_device,
        mesh=split,
        in_specs=(
            P(ALL, None, None),
            P(ALL),
            P(ALL),
            P(ALL),
            P(ALL),
            P(ALL),
            P(),
            P(),
            P(),
        ),
        out_specs=(P(), P(ALL), P()),
        check_vma=False,
    )
```

```python
import jax
import jax.numpy as jnp
from jax import lax
from jax.experimental import pallas as pl
from jax.experimental.pallas import tpu as pltpu
from jax.sharding import Mesh
from jax.sharding import PartitionSpec as P

ITERS = 3
STEP = 0.3
TINY = 1e-06
BLOCKS = 32
SLOTS = 80
TR = 128
CB = 1024
COL_BLOCKS = 256
ROWS_P = 2048
CHIPS = 64
SHARE = 16
CHUNK = 8
CHUNKS = SLOTS // CHUNK
ON_MXU = 2

CHIP = ("grp", "dev_0", "dev_1")
CORE = "dev_2"
ALL = ("grp", "dev_0", "dev_1", "dev_2")
SWAP = [(0, 1), (1, 0)]
MIB = 1 << 20
FIRST_LIMIT = 48
PASS_LIMIT = 48

f32 = jnp.float32
bf16 = jnp.bfloat16


def round_bf16(x):
    return x.astype(bf16).astype(f32)


def find_owners(count_ref, owner_ref):
    def clear(s, carry):
        owner_ref[s] = BLOCKS
        return carry

    def block(b, start):
        stop = start + count_ref[b]

        def slot(s, carry):
            owner_ref[s] = b
            return carry

        return lax.fori_loop(start, stop, slot, start) * 0 + stop

    lax.fori_loop(0, SLOTS, clear, 0)
    lax.fori_loop(0, BLOCKS, block, 0)


def row_tiles(slots, column_ref, owner_ref, tile_ref, table_ref, image_ref):
    results = []
    for u, s in enumerate(slots):
        col = column_ref[s]
        parts = [
            jnp.broadcast_to(table_ref[col, pl.ds(part, 1), :], (8, 128)) for part in range(8)
        ]
        if u < ON_MXU:
            left = jnp.concatenate(parts, axis=1).astype(bf16)
            r = 0.125 * lax.dot_general(
                left, tile_ref[s], (((1,), (1,)), ((), ())), preferred_element_type=f32
            )
        else:
            sums = []
            for g in range(TR // 8):
                rows = tile_ref[s, pl.ds(8 * g, 8), :].astype(f32)
                total = rows[:, 0:128] * parts[0]
                for part in range(1, 8):
                    total = total + rows[:, 128 * part : 128 * part + 128] * parts[part]
                sums.append(total)
            r = jnp.sum(jnp.concatenate(sums, axis=0).T.reshape(16, 8, 128), axis=0)
        results.append(r)
    for s, r in zip(slots, results):
        image_ref[owner_ref[s]] += r


def image_rows(image_ref):
    return jnp.concatenate(
        [jnp.sum(image_ref[b], axis=0, keepdims=True) for b in range(BLOCKS)], axis=0
    )


def column_tiles(slots, lefts, column_ref, tile_ref, sum_ref):
    sub = lax.broadcasted_iota(jnp.int32, (8, 128), 0)
    results = []
    for s, left in zip(slots, lefts):
        left = jnp.broadcast_to(left, (8, TR)).astype(bf16)
        out = jnp.dot(left, tile_ref[s], preferred_element_type=f32)
        r = out[:, 0:128]
        for part in range(1, 8):
            r = jnp.where(sub == part, out[:, 128 * part : 128 * part + 128], r)
        results.append(r)
    for s, r in zip(slots, results):
        sum_ref[column_ref[s]] += r


def clear_blocks(ref):
    n = ref.shape[0]

    def clear(i, carry):
        ref[i] = jnp.zeros((8, 128), f32)
        return carry

    lax.fori_loop(0, n, clear, 0, unroll=8 if n % 8 == 0 else 3)


def put_sums(sum_ref, core, own_ref, other_ref, scalars):
    def put(i, carry):
        for ref, side in ((own_ref, core), (other_ref, 1 - core)):
            at = side * (COL_BLOCKS // 2) + 2 * i
            ref[i, pl.ds(0, 8), :] = sum_ref[at]
            ref[i, pl.ds(8, 8), :] = sum_ref[at + 1]
            if scalars is not None:
                ref[i, pl.ds(SHARE, 8), :] = scalars
        return carry

    lax.fori_loop(0, CHIPS, put, 0, unroll=4)


def chunk_of(i):
    return [i * CHUNK + u for u in range(CHUNK)]


def tile_copies(tiles_hbm, tile_ref, sem):
    def chunk(i):
        return pltpu.make_async_copy(
            tiles_hbm.at[pl.ds(i * CHUNK, CHUNK)], tile_ref.at[pl.ds(i * CHUNK, CHUNK)], sem.at[i]
        )

    for i in range(CHUNKS):
        chunk(i).start()
    return chunk


def first_kernel(
    count_hbm, column_hbm, place_ref, tiles_hbm, dual_hbm, primal_hbm,
    owner_ref, image_out, own_ref, other_ref,
    count_ref, column_ref, dual_ref, wide_ref, table_ref, tile_ref, sum_ref, image_ref,
    tile_sem, side_sem,
):
    sides = [
        pltpu.make_async_copy(src, dst, side_sem.at[i])
        for i, (src, dst) in enumerate(
            (
                (count_hbm, count_ref),
                (column_hbm, column_ref),
                (dual_hbm, dual_ref),
                (primal_hbm, table_ref),
            )
        )
    ]
    for copy in sides:
        copy.start()
    arriving = tile_copies(tiles_hbm, tile_ref, tile_sem)
    clear_blocks(sum_ref)
    clear_blocks(image_ref)
    for copy in sides:
        copy.wait()
    find_owners(count_ref, owner_ref)
    wide_ref[pl.ds(0, BLOCKS), :] = dual_ref[...].astype(f32)
    wide_ref[pl.ds(BLOCKS, 8), :] = jnp.zeros((8, TR), f32)

    def fill(i, carry):
        table_ref[i] = round_bf16(table_ref[i])
        return carry

    lax.fori_loop(0, COL_BLOCKS, fill, 0, unroll=8)

    def step(i, carry):
        arriving(i).wait()
        slots = chunk_of(i)
        row_tiles(slots, column_ref, owner_ref, tile_ref, table_ref, image_ref)
        lefts = [wide_ref[pl.ds(owner_ref[s], 1), :] for s in slots]
        column_tiles(slots, lefts, column_ref, tile_ref, sum_ref)
        return carry

    lax.fori_loop(0, CHUNKS, step, 0)
    image_out[...] = image_rows(image_ref)
    put_sums(sum_ref, place_ref[0], own_ref, other_ref, None)


def merge_kernel(own_ref, other_ref, out_ref):
    def add(i, carry):
        out_ref[i] = own_ref[i] + other_ref[i]
        return carry

    lax.fori_loop(0, CHIPS, add, 0, unroll=8)


def fill_table(own_ref, other_ref, core, table_ref):
    def fill(i, carry):
        for ref, side in ((own_ref, core), (other_ref, 1 - core)):
            part = ref[i].astype(f32) if ref.dtype == bf16 else round_bf16(ref[i])
            at = side * (COL_BLOCKS // 2) + 2 * i
            table_ref[at] = part[0:8]
            table_ref[at + 1] = part[8:16]
        return carry

    lax.fori_loop(0, CHIPS, fill, 0, unroll=4)


def dual_step(bounds_ref, dual_in, image_before, image, change_in, sigma):
    bounds = bounds_ref[...]
    dual = jnp.maximum(
        dual_in[...] + sigma * (bounds - (2.0 * image - image_before)), 0.0
    )
    short = jnp.maximum(bounds - image, 0.0)
    violation = jnp.sum(short * short)
    lane = lax.broadcasted_iota(jnp.int32, (8, 128), 1)
    scalars = jnp.where(lane == 0, violation, jnp.where(lane == 1, change_in[...], 0.0))
    return dual, scalars


def middle_kernel(
    column_ref, owner_ref, place_ref, tiles_hbm, own_in, other_in, bounds_ref, dual_in,
    before_ref, change_in, sigma_in,
    dual_ref, image_out, own_ref, other_ref,
    table_ref, tile_ref, sum_ref, image_ref, tile_sem,
):
    core = place_ref[0]
    arriving = tile_copies(tiles_hbm, tile_ref, tile_sem)
    fill_table(own_in, other_in, core, table_ref)
    clear_blocks(sum_ref)
    clear_blocks(image_ref)
    sigma = sigma_in[0:1, :]

    def rows(i):
        arriving(i).wait()
        row_tiles(chunk_of(i), column_ref, owner_ref, tile_ref, table_ref, image_ref)

    def left(s):
        b = owner_ref[s]
        at = pl.ds(jnp.minimum(b, BLOCKS - 1), 1)
        image = jnp.sum(image_ref[b], axis=0, keepdims=True)
        move = bounds_ref[at, :] - (2.0 * image - before_ref[at, :])
        row = jnp.maximum(dual_in[at, :] + sigma * move, 0.0)
        return jnp.where(b < BLOCKS, row, 0.0)

    def columns(slots):
        column_tiles(slots, [left(s) for s in slots], column_ref, tile_ref, sum_ref)

    def early(i, carry):
        rows(i)
        return carry

    def step(i, carry):
        columns(chunk_of(i - 2))
        rows(i)
        return carry

    lax.fori_loop(0, 2, early, 0)
    lax.fori_loop(2, CHUNKS, step, 0)
    columns(chunk_of(CHUNKS - 2) + chunk_of(CHUNKS - 1))
    image = image_rows(image_ref)
    dual, scalars = dual_step(bounds_ref, dual_in, before_ref[...], image, change_in, sigma)
    image_out[...] = image
    dual_ref[...] = dual
    put_sums(sum_ref, core, own_ref, other_ref, scalars)


def last_kernel(
    column_ref, owner_ref, place_ref, target_ref, tiles_hbm, own_in, other_in, bounds_ref,
    dual_in, before_ref, change_in, sigma_in,
    primal_ref, send_ref,
    table_ref, tile_ref, image_ref, tile_sem,
):
    core = place_ref[0]
    arriving = tile_copies(tiles_hbm, tile_ref, tile_sem)
    fill_table(own_in, other_in, core, table_ref)
    clear_blocks(image_ref)

    def lay(i, carry):
        for ref, side in ((own_in, core), (other_in, 1 - core)):
            at = pl.multiple_of((side * CHIPS + i) * SHARE, SHARE)
            primal_ref[pl.ds(at, SHARE), :] = ref[i]
        return carry

    lax.fori_loop(0, CHIPS, lay, 0, unroll=4)

    def step(i, carry):
        arriving(i).wait()
        row_tiles(chunk_of(i), column_ref, owner_ref, tile_ref, table_ref, image_ref)
        return carry

    lax.fori_loop(0, CHUNKS, step, 0)
    dual, scalars = dual_step(
        bounds_ref, dual_in, before_ref[...], image_rows(image_ref), change_in, sigma_in[0:1, :]
    )

    def put(i, carry):
        send_ref[i] = scalars
        return carry

    lax.fori_loop(0, CHIPS, put, 0, unroll=8)
    first = place_ref[2] * (BLOCKS // 2)
    for b in range(BLOCKS):
        to = target_ref[b]
        send_ref[first + jnp.right_shift(to, 1), pl.ds(jnp.bitwise_and(to, 1), 1), :] = dual[
            b : b + 1, :
        ]


def next_weight(weight, scalars):
    lane = lax.broadcasted_iota(jnp.int32, (8, 128), 1)
    violation = jnp.sum(jnp.where(lane == 0, scalars, 0.0), axis=1, keepdims=True)
    change = jnp.sum(jnp.where(lane == 1, scalars, 0.0), axis=1, keepdims=True)
    ratio = jnp.broadcast_to((violation + TINY) / (change + TINY), (8, 128))
    return jnp.sqrt(weight * jnp.sqrt(ratio))


def update_kernel(first, *refs):
    if first:
        (arrived_ref, place_ref, primal_full, cost_full, upper_full,
         primal_ref, send_ref, change_ref, weight_ref, sigma_ref, cost_ref, upper_ref) = refs
        at = pl.ds(pl.multiple_of(place_ref[1] * SHARE, SHARE), SHARE)
        primal, cost, upper = primal_full[at, :], cost_full[at, :], upper_full[at, :]
        cost_ref[...] = cost
        upper_ref[...] = upper
    else:
        (arrived_ref, primal_in, cost_in, upper_in, weight_in,
         primal_ref, send_ref, change_ref, weight_ref, sigma_ref) = refs
        primal, cost, upper = primal_in[...], cost_in[...], upper_in[...]
    rows = arrived_ref.shape[1]

    def add(i, total):
        return total + arrived_ref[i]

    total = lax.fori_loop(0, CHIPS, add, jnp.zeros((rows, 128), f32), unroll=8)
    if first:
        weight = jnp.ones((8, 128), f32)
    else:
        weight = next_weight(weight_in[...], total[SHARE:, :])
    tau = STEP / weight[0:1, :]
    new = jnp.clip(primal - tau * (cost - total[:SHARE, :]), 0.0, upper)
    primal_ref[...] = new
    moved = new - primal
    change_ref[...] = jnp.full((8, 128), jnp.sum(moved * moved), f32)
    weight_ref[...] = weight
    sigma_ref[...] = STEP * weight
    out = new.astype(send_ref.dtype)

    def put(i, carry):
        send_ref[i] = out
        return carry

    lax.fori_loop(0, CHIPS, put, 0, unroll=8)


def finish_kernel(place_ref, same_ref, cross_ref, weight_in, dual_ref, weight_ref):
    def add(i, total):
        return total + (same_ref[i] + cross_ref[i])

    total = lax.fori_loop(0, CHIPS, add, jnp.zeros((8, 128), f32), unroll=8)
    total = jnp.broadcast_to(total[2:3, :], (8, 128))
    weight_ref[...] = next_weight(weight_in[...], total)
    core = place_ref[0]
    first = place_ref[2] * (BLOCKS // 2)
    for chip in range(BLOCKS // 2):
        same = same_ref[first + chip, pl.ds(core, 1), :]
        cross = cross_ref[first + chip, pl.ds(core, 1), :]
        dual_ref[pl.ds(2 * chip + core, 1), :] = same
        dual_ref[pl.ds(2 * chip + 1 - core, 1), :] = cross


SMEM = pl.BlockSpec(memory_space=pltpu.SMEM)
VMEM = pl.BlockSpec(memory_space=pltpu.VMEM)
ANY = pl.BlockSpec(memory_space=pl.ANY)


def sds(shape, dtype=f32):
    return jax.ShapeDtypeStruct(shape, dtype)


def call(kernel, name, in_specs, out_shape, out_specs, scratch=(), limit=8):
    return pl.pallas_call(
        kernel,
        name=name,
        in_specs=in_specs,
        out_specs=out_specs,
        out_shape=out_shape,
        scratch_shapes=list(scratch),
        compiler_params=pltpu.CompilerParams(vmem_limit_bytes=limit * MIB),
    )


TILE = pltpu.VMEM((SLOTS, TR, CB), bf16)
TABLE = pltpu.VMEM((COL_BLOCKS, 8, 128), f32)
IMAGE = pltpu.VMEM((BLOCKS + 1, 8, 128), f32)
DMA = pltpu.SemaphoreType.DMA


def summed(own, other):
    crossed = lax.ppermute(other, CORE, SWAP)
    merged = call(merge_kernel, "merge", [VMEM] * 2, sds(own.shape), VMEM, limit=4)(own, crossed)
    return lax.all_to_all(merged, CHIP, 0, 0, tiled=True)


def gathered(send):
    own = lax.all_to_all(send, CHIP, 0, 0, tiled=True)
    return own, lax.ppermute(own, CORE, SWAP)


def per_device(
    matrix_tiles,
    tile_column,
    block_counts,
    destination,
    row_bounds,
    dual_start,
    primal_start,
    cost_vector,
    upper_bound,
):
    core = lax.axis_index(CORE)
    place = jnp.stack(
        [core, core * CHIPS + lax.axis_index(CHIP), lax.axis_index("grp")]
    ).astype(jnp.int32)
    bounds = row_bounds.astype(f32).reshape(BLOCKS, TR)
    dual_bf = dual_start.reshape(BLOCKS, TR)
    dual = dual_bf.astype(f32)
    wide = (ROWS_P, 128)
    part = sds((SHARE, 128))
    tiny = sds((8, 128))

    owners, before, own, other = call(
        first_kernel,
        "first_pass",
        [ANY, ANY, SMEM, ANY, ANY, ANY],
        (
            sds((SLOTS,), jnp.int32),
            sds((BLOCKS, TR)),
            sds((CHIPS, SHARE, 128)),
            sds((CHIPS, SHARE, 128)),
        ),
        (SMEM, VMEM, VMEM, VMEM),
        (
            pltpu.SMEM((BLOCKS,), jnp.int32),
            pltpu.SMEM((SLOTS,), jnp.int32),
            pltpu.VMEM((BLOCKS, TR), bf16),
            pltpu.VMEM((BLOCKS + 8, TR), f32),
            TABLE,
            TILE,
            TABLE,
            IMAGE,
            DMA((CHUNKS,)),
            DMA((4,)),
        ),
        limit=FIRST_LIMIT,
    )(
        block_counts, tile_column, place, matrix_tiles, dual_bf,
        primal_start.reshape(COL_BLOCKS, 8, 128),
    )

    for iteration in range(ITERS):
        first, last = iteration == 0, iteration == ITERS - 1
        arrived = summed(own, other)
        send_shape = sds((CHIPS, SHARE, 128), f32 if last else bf16)
        if first:
            primal, send, change, weight, sigma, cost, upper = call(
                lambda *refs: update_kernel(True, *refs),
                "update",
                [VMEM, SMEM] + [VMEM] * 3,
                (part, send_shape, tiny, tiny, tiny, part, part),
                (VMEM,) * 7,
                limit=4,
            )(
                arrived, place, primal_start.reshape(wide), cost_vector.reshape(wide),
                upper_bound.reshape(wide),
            )
        else:
            primal, send, change, weight, sigma = call(
                lambda *refs: update_kernel(False, *refs),
                "update",
                [VMEM] * 5,
                (part, send_shape, tiny, tiny, tiny),
                (VMEM,) * 5,
                limit=4,
            )(arrived, primal, cost, upper, weight)
        near, far = gathered(send)
        if last:
            break
        dual, before, own, other = call(
            middle_kernel,
            "middle_pass",
            [SMEM] * 3 + [ANY] + [VMEM] * 7,
            (sds((BLOCKS, TR)), sds((BLOCKS, TR)))
            + (sds((CHIPS, SHARE + 8, 128)),) * 2,
            (VMEM,) * 4,
            (TABLE, TILE, TABLE, IMAGE, DMA((CHUNKS,))),
            limit=PASS_LIMIT,
        )(
            tile_column, owners, place, matrix_tiles, near, far, bounds, dual, before, change,
            sigma,
        )
    primal_final, send = call(
        last_kernel,
        "last_pass",
        [SMEM] * 4 + [ANY] + [VMEM] * 7,
        (sds(wide), sds((CHIPS, 8, 128))),
        (VMEM,) * 2,
        (TABLE, TILE, IMAGE, DMA((CHUNKS,))),
        limit=PASS_LIMIT,
    )(
        tile_column, owners, place, destination, matrix_tiles, near, far, bounds, dual, before, change,
        sigma,
    )
    same, cross = gathered(send)
    dual_final, weight = call(
        finish_kernel,
        "finish",
        [SMEM, VMEM, VMEM, VMEM],
        (sds((BLOCKS, TR)), tiny),
        (VMEM, VMEM),
        limit=4,
    )(place, same, cross, weight)
    return (primal_final.reshape(-1), dual_final.reshape(-1), weight[0, 0:1])


def solution(mesh):
    split = Mesh(
        mesh.devices.reshape(mesh.shape["grp"], 4, 4, 2), ("grp", "dev_0", "dev_1", "dev_2")
    )
    return jax.shard_map(
        per_device,
        mesh=split,
        in_specs=(
            P(ALL, None, None),
            P(ALL),
            P(ALL),
            P(ALL),
            P(ALL),
            P(ALL),
            P(),
            P(),
            P(),
        ),
        out_specs=(P(), P(ALL), P()),
        check_vma=False,
    )
```

```python
import jax
import jax.numpy as jnp
from jax import lax
from jax.experimental import pallas as pl
from jax.experimental.pallas import tpu as pltpu
from jax.sharding import Mesh
from jax.sharding import PartitionSpec as P

ITERS = 3
STEP = 0.3
TINY = 1e-06
BLOCKS = 32
SLOTS = 80
TR = 128
CB = 1024
COL_BLOCKS = 256
ROWS_P = 2048
CHIPS = 64
SHARE = 16
CHUNK = 8
CHUNKS = SLOTS // CHUNK
ON_MXU = 2

CHIP = ("grp", "dev_0", "dev_1")
CORE = "dev_2"
ALL = ("grp", "dev_0", "dev_1", "dev_2")
SWAP = [(0, 1), (1, 0)]
MIB = 1 << 20
PASS_LIMIT = 48

f32 = jnp.float32
bf16 = jnp.bfloat16


def round_bf16(x):
    return x.astype(bf16).astype(f32)


def find_owners(count_ref, owner_ref):
    def clear(s, carry):
        owner_ref[s] = BLOCKS
        return carry

    def block(b, start):
        stop = start + count_ref[b]

        def slot(s, carry):
            owner_ref[s] = b
            return carry

        return lax.fori_loop(start, stop, slot, start) * 0 + stop

    lax.fori_loop(0, SLOTS, clear, 0)
    lax.fori_loop(0, BLOCKS, block, 0)


def row_tile(u, s, column_ref, tiles, table_ref):
    col = column_ref[s]
    parts = [jnp.broadcast_to(table_ref[col, pl.ds(part, 1), :], (8, 128)) for part in range(8)]
    if u < ON_MXU:
        left = jnp.concatenate(parts, axis=1).astype(bf16)
        return 0.125 * lax.dot_general(
            left, tiles[s], (((1,), (1,)), ((), ())), preferred_element_type=f32
        )
    sums = []
    for g in range(TR // 8):
        rows = tiles[s, pl.ds(8 * g, 8), slice(None)].astype(f32)
        total = rows[:, 0:128] * parts[0]
        for part in range(1, 8):
            total = total + rows[:, 128 * part : 128 * part + 128] * parts[part]
        sums.append(total)
    return jnp.sum(jnp.concatenate(sums, axis=0).T.reshape(16, 8, 128), axis=0)


def row_chunk(i, arrive, column_ref, owner_ref, tiles, table_ref, image_ref):
    arrive(i)
    results = [row_tile(u, s, column_ref, tiles, table_ref) for u, s in enumerate(chunk_of(i))]
    for s, r in zip(chunk_of(i), results):
        image_ref[owner_ref[s]] += r


def image_rows(image_ref):
    return jnp.concatenate(
        [jnp.sum(image_ref[b], axis=0, keepdims=True) for b in range(BLOCKS)], axis=0
    )


def column_tiles(slots, lefts, column_ref, tiles, sum_ref):
    sub = lax.broadcasted_iota(jnp.int32, (8, 128), 0)
    results = []
    for s, left in zip(slots, lefts):
        left = jnp.broadcast_to(left, (8, TR)).astype(bf16)
        out = jnp.dot(left, tiles[s], preferred_element_type=f32)
        r = out[:, 0:128]
        for part in range(1, 8):
            r = jnp.where(sub == part, out[:, 128 * part : 128 * part + 128], r)
        results.append(r)
    for s, r in zip(slots, results):
        sum_ref[column_ref[s]] += r


def clear_blocks(ref):
    n = ref.shape[0]

    def clear(i, carry):
        ref[i] = jnp.zeros((8, 128), f32)
        return carry

    lax.fori_loop(0, n, clear, 0, unroll=8 if n % 8 == 0 else 3)


def put_sums(sum_ref, core, own_ref, other_ref, scalars):
    def put(i, carry):
        for ref, side in ((own_ref, core), (other_ref, 1 - core)):
            at = side * (COL_BLOCKS // 2) + 2 * i
            ref[i, pl.ds(0, 8), :] = sum_ref[at]
            ref[i, pl.ds(8, 8), :] = sum_ref[at + 1]
            if scalars is not None:
                ref[i, pl.ds(SHARE, 8), :] = scalars
        return carry

    lax.fori_loop(0, CHIPS, put, 0, unroll=4)


def chunk_of(i):
    return [i * CHUNK + u for u in range(CHUNK)]


def start_tiles(tiles_hbm, kept_ref, tile_ref, sem, first):
    copies = {}
    for i in range(0 if first else 1, CHUNKS):
        to = kept_ref if i == 0 else tile_ref.at[pl.ds((i - 1) * CHUNK, CHUNK)]
        copies[i] = pltpu.make_async_copy(tiles_hbm.at[pl.ds(i * CHUNK, CHUNK)], to, sem.at[i])
        copies[i].start()

    def arrive(i):
        if i in copies:
            copies[i].wait()

    return arrive


class Tiles:
    def __init__(self, kept_ref, tile_ref):
        self.refs = kept_ref, tile_ref

    def __getitem__(self, at):
        s = at[0] if isinstance(at, tuple) else at
        rest = at[1:] if isinstance(at, tuple) else ()
        ref, base = (self.refs[0], 0) if s < CHUNK else (self.refs[1], CHUNK)
        return ref[(s - base, *rest)]


def first_kernel(
    count_hbm, column_hbm, place_ref, tiles_hbm, dual_hbm, primal_hbm,
    owner_ref, image_out, own_ref, other_ref, kept_ref,
    count_ref, column_ref, dual_ref, wide_ref, table_ref, tile_ref, sum_ref, image_ref,
    tile_sem, side_sem,
):
    sides = [
        pltpu.make_async_copy(src, dst, side_sem.at[i])
        for i, (src, dst) in enumerate(
            (
                (count_hbm, count_ref),
                (column_hbm, column_ref),
                (dual_hbm, dual_ref),
                (primal_hbm, table_ref),
            )
        )
    ]
    for copy in sides:
        copy.start()
    arrive = start_tiles(tiles_hbm, kept_ref, tile_ref, tile_sem, True)
    tiles = Tiles(kept_ref, tile_ref)
    clear_blocks(sum_ref)
    clear_blocks(image_ref)
    for copy in sides:
        copy.wait()
    find_owners(count_ref, owner_ref)
    wide_ref[pl.ds(0, BLOCKS), :] = dual_ref[...].astype(f32)
    wide_ref[pl.ds(BLOCKS, 8), :] = jnp.zeros((8, TR), f32)

    def fill(i, carry):
        table_ref[i] = round_bf16(table_ref[i])
        return carry

    lax.fori_loop(0, COL_BLOCKS, fill, 0, unroll=8)

    for i in range(CHUNKS):
        row_chunk(i, arrive, column_ref, owner_ref, tiles, table_ref, image_ref)
        lefts = [wide_ref[pl.ds(owner_ref[s], 1), :] for s in chunk_of(i)]
        column_tiles(chunk_of(i), lefts, column_ref, tiles, sum_ref)
    image_out[...] = image_rows(image_ref)
    put_sums(sum_ref, place_ref[0], own_ref, other_ref, None)


def merge_kernel(own_ref, other_ref, out_ref):
    rows = own_ref.shape[1]
    if rows > SHARE:
        rest = own_ref[0, pl.ds(SHARE, 8), :] + other_ref[0, pl.ds(SHARE, 8), :]
        sub = lax.broadcasted_iota(jnp.int32, (8, 128), 0)
        parts = jnp.zeros((8, 128), f32)
        for p in range(3):
            head = round_bf16(rest)
            parts = jnp.where(sub == p, head, parts)
            rest = rest - head
        parts = parts.astype(bf16)

    def add(i, carry):
        data = pl.ds(0, SHARE)
        out_ref[i, data, :] = (own_ref[i, data, :] + other_ref[i, data, :]).astype(bf16)
        if rows > SHARE:
            out_ref[i, pl.ds(SHARE, 8), :] = parts
        return carry

    lax.fori_loop(0, CHIPS, add, 0, unroll=8)


def fill_table(own_ref, other_ref, core, table_ref):
    def fill(i, carry):
        for ref, side in ((own_ref, core), (other_ref, 1 - core)):
            part = ref[i].astype(f32) if ref.dtype == bf16 else round_bf16(ref[i])
            at = side * (COL_BLOCKS // 2) + 2 * i
            table_ref[at] = part[0:8]
            table_ref[at + 1] = part[8:16]
        return carry

    lax.fori_loop(0, CHIPS, fill, 0, unroll=4)


def dual_step(bounds_ref, dual_in, image_before, image, change_in, sigma):
    bounds = bounds_ref[...]
    dual = jnp.maximum(
        dual_in[...] + sigma * (bounds - (2.0 * image - image_before)), 0.0
    )
    short = jnp.maximum(bounds - image, 0.0)
    violation = jnp.sum(short * short)
    lane = lax.broadcasted_iota(jnp.int32, (8, 128), 1)
    scalars = jnp.where(lane == 0, violation, jnp.where(lane == 1, change_in[...], 0.0))
    return dual, scalars


def middle_kernel(
    column_ref, owner_ref, place_ref, tiles_hbm, kept_ref, own_in, other_in, bounds_ref, dual_in,
    before_ref, change_in, sigma_in,
    dual_ref, image_out, own_ref, other_ref,
    table_ref, tile_ref, sum_ref, image_ref, tile_sem,
):
    core = place_ref[0]
    arrive = start_tiles(tiles_hbm, kept_ref, tile_ref, tile_sem, False)
    tiles = Tiles(kept_ref, tile_ref)
    fill_table(own_in, other_in, core, table_ref)
    clear_blocks(sum_ref)
    clear_blocks(image_ref)
    sigma = sigma_in[0:1, :]

    def left(s):
        b = owner_ref[s]
        at = pl.ds(jnp.minimum(b, BLOCKS - 1), 1)
        image = jnp.sum(image_ref[b], axis=0, keepdims=True)
        move = bounds_ref[at, :] - (2.0 * image - before_ref[at, :])
        row = jnp.maximum(dual_in[at, :] + sigma * move, 0.0)
        return jnp.where(b < BLOCKS, row, 0.0)

    done = 0
    for i in range(CHUNKS + 1):
        ready = SLOTS if i == CHUNKS else max(i * CHUNK - 4, 0)
        slots = range(done, ready)
        lefts = [left(s) for s in slots]
        if i < CHUNKS:
            row_chunk(i, arrive, column_ref, owner_ref, tiles, table_ref, image_ref)
        column_tiles(slots, lefts, column_ref, tiles, sum_ref)
        done = ready
    image = image_rows(image_ref)
    dual, scalars = dual_step(bounds_ref, dual_in, before_ref[...], image, change_in, sigma)
    image_out[...] = image
    dual_ref[...] = dual
    put_sums(sum_ref, core, own_ref, other_ref, scalars)


def last_kernel(
    column_ref, owner_ref, place_ref, target_ref, tiles_hbm, kept_ref, own_in, other_in, bounds_ref,
    dual_in, before_ref, change_in, sigma_in,
    primal_ref, send_ref,
    table_ref, tile_ref, image_ref, tile_sem,
):
    core = place_ref[0]
    arrive = start_tiles(tiles_hbm, kept_ref, tile_ref, tile_sem, False)
    tiles = Tiles(kept_ref, tile_ref)
    fill_table(own_in, other_in, core, table_ref)
    clear_blocks(image_ref)

    def lay(i, carry):
        for ref, side in ((own_in, core), (other_in, 1 - core)):
            at = pl.multiple_of((side * CHIPS + i) * SHARE, SHARE)
            primal_ref[pl.ds(at, SHARE), :] = ref[i]
        return carry

    lax.fori_loop(0, CHIPS, lay, 0, unroll=4)

    for i in range(CHUNKS):
        row_chunk(i, arrive, column_ref, owner_ref, tiles, table_ref, image_ref)
    dual, scalars = dual_step(
        bounds_ref, dual_in, before_ref[...], image_rows(image_ref), change_in, sigma_in[0:1, :]
    )

    def put(i, carry):
        send_ref[i] = scalars
        return carry

    lax.fori_loop(0, CHIPS, put, 0, unroll=8)
    first = place_ref[2] * (BLOCKS // 2)
    for b in range(BLOCKS):
        to = target_ref[b]
        send_ref[first + jnp.right_shift(to, 1), pl.ds(jnp.bitwise_and(to, 1), 1), :] = dual[
            b : b + 1, :
        ]


def next_weight(weight, scalars):
    lane = lax.broadcasted_iota(jnp.int32, (8, 128), 1)
    violation = jnp.sum(jnp.where(lane == 0, scalars, 0.0), axis=1, keepdims=True)
    change = jnp.sum(jnp.where(lane == 1, scalars, 0.0), axis=1, keepdims=True)
    ratio = jnp.broadcast_to((violation + TINY) / (change + TINY), (8, 128))
    return jnp.sqrt(weight * jnp.sqrt(ratio))


def update_kernel(first, *refs):
    if first:
        (arrived_ref, place_ref, primal_full, cost_full, upper_full,
         primal_ref, send_ref, change_ref, weight_ref, sigma_ref, cost_ref, upper_ref) = refs
        at = pl.ds(pl.multiple_of(place_ref[1] * SHARE, SHARE), SHARE)
        primal, cost, upper = primal_full[at, :], cost_full[at, :], upper_full[at, :]
        cost_ref[...] = cost
        upper_ref[...] = upper
    else:
        (arrived_ref, primal_in, cost_in, upper_in, weight_in,
         primal_ref, send_ref, change_ref, weight_ref, sigma_ref) = refs
        primal, cost, upper = primal_in[...], cost_in[...], upper_in[...]
    rows = arrived_ref.shape[1]

    def add(i, total):
        return total + arrived_ref[i].astype(f32)

    total = lax.fori_loop(0, CHIPS, add, jnp.zeros((rows, 128), f32), unroll=8)
    if first:
        weight = jnp.ones((8, 128), f32)
    else:
        scalars = total[SHARE : SHARE + 1, :] + total[SHARE + 1 : SHARE + 2, :]
        scalars = scalars + total[SHARE + 2 : SHARE + 3, :]
        weight = next_weight(weight_in[...], jnp.broadcast_to(scalars, (8, 128)))
    tau = STEP / weight[0:1, :]
    new = jnp.clip(primal - tau * (cost - total[:SHARE, :]), 0.0, upper)
    primal_ref[...] = new
    moved = new - primal
    change_ref[...] = jnp.full((8, 128), jnp.sum(moved * moved), f32)
    weight_ref[...] = weight
    sigma_ref[...] = STEP * weight
    out = new.astype(send_ref.dtype)

    def put(i, carry):
        send_ref[i] = out
        return carry

    lax.fori_loop(0, CHIPS, put, 0, unroll=8)


def finish_kernel(place_ref, same_ref, cross_ref, weight_in, dual_ref, weight_ref):
    def add(i, total):
        return total + (same_ref[i] + cross_ref[i])

    total = lax.fori_loop(0, CHIPS, add, jnp.zeros((8, 128), f32), unroll=8)
    total = jnp.broadcast_to(total[2:3, :], (8, 128))
    weight_ref[0] = next_weight(weight_in[...], total)[0, 0]
    core = place_ref[0]
    first = place_ref[2] * (BLOCKS // 2)
    for chip in range(BLOCKS // 2):
        same = same_ref[first + chip, pl.ds(core, 1), :]
        cross = cross_ref[first + chip, pl.ds(core, 1), :]
        dual_ref[pl.ds(2 * chip + core, 1), :] = same
        dual_ref[pl.ds(2 * chip + 1 - core, 1), :] = cross


SMEM = pl.BlockSpec(memory_space=pltpu.SMEM)
VMEM = pl.BlockSpec(memory_space=pltpu.VMEM)
ANY = pl.BlockSpec(memory_space=pl.ANY)


def sds(shape, dtype=f32):
    return jax.ShapeDtypeStruct(shape, dtype)


def call(kernel, name, in_specs, out_shape, out_specs, scratch=(), limit=8):
    return pl.pallas_call(
        kernel,
        name=name,
        in_specs=in_specs,
        out_specs=out_specs,
        out_shape=out_shape,
        scratch_shapes=list(scratch),
        compiler_params=pltpu.CompilerParams(vmem_limit_bytes=limit * MIB),
    )


TILE = pltpu.VMEM((SLOTS - CHUNK, TR, CB), bf16)
TABLE = pltpu.VMEM((COL_BLOCKS, 8, 128), f32)
IMAGE = pltpu.VMEM((BLOCKS + 1, 8, 128), f32)
DMA = pltpu.SemaphoreType.DMA


def first_call(*args):
    return call(
        first_kernel,
        "first_pass",
        [ANY, ANY, SMEM, ANY, ANY, ANY],
        (
            sds((SLOTS,), jnp.int32),
            sds((BLOCKS, TR)),
            sds((CHIPS, SHARE, 128)),
            sds((CHIPS, SHARE, 128)),
            sds((CHUNK, TR, CB), bf16),
        ),
        (SMEM, VMEM, VMEM, VMEM, VMEM),
        (
            pltpu.SMEM((BLOCKS,), jnp.int32),
            pltpu.SMEM((SLOTS,), jnp.int32),
            pltpu.VMEM((BLOCKS, TR), bf16),
            pltpu.VMEM((BLOCKS + 8, TR), f32),
            TABLE,
            TILE,
            TABLE,
            IMAGE,
            DMA((CHUNKS,)),
            DMA((4,)),
        ),
        limit=PASS_LIMIT,
    )(*args)


def middle_call(*args):
    return call(
        middle_kernel,
        "middle_pass",
        [SMEM] * 3 + [ANY] + [VMEM] * 8,
        (sds((BLOCKS, TR)), sds((BLOCKS, TR))) + (sds((CHIPS, SHARE + 8, 128)),) * 2,
        (VMEM,) * 4,
        (TABLE, TILE, TABLE, IMAGE, DMA((CHUNKS,))),
        limit=PASS_LIMIT,
    )(*args)


def last_call(*args):
    return call(
        last_kernel,
        "last_pass",
        [SMEM] * 4 + [ANY] + [VMEM] * 8,
        (sds((ROWS_P, 128)), sds((CHIPS, 8, 128))),
        (VMEM,) * 2,
        (TABLE, TILE, IMAGE, DMA((CHUNKS,))),
        limit=PASS_LIMIT,
    )(*args)


def summed(own, other):
    crossed = lax.ppermute(other, CORE, SWAP)
    merged = call(merge_kernel, "merge", [VMEM] * 2, sds(own.shape, bf16), VMEM, limit=4)(
        own, crossed
    )
    return lax.all_to_all(merged, CHIP, 0, 0, tiled=True)


def gathered(send):
    own = lax.all_to_all(send, CHIP, 0, 0, tiled=True)
    return own, lax.ppermute(own, CORE, SWAP)


def per_device(
    matrix_tiles,
    tile_column,
    block_counts,
    destination,
    row_bounds,
    dual_start,
    primal_start,
    cost_vector,
    upper_bound,
):
    core = lax.axis_index(CORE)
    place = jnp.stack(
        [core, core * CHIPS + lax.axis_index(CHIP), lax.axis_index("grp")]
    ).astype(jnp.int32)
    bounds = row_bounds.astype(f32).reshape(BLOCKS, TR)
    dual_bf = dual_start.reshape(BLOCKS, TR)
    dual = dual_bf.astype(f32)
    wide = (ROWS_P, 128)
    part = sds((SHARE, 128))
    tiny = sds((8, 128))

    owners, before, own, other, kept = first_call(
        block_counts, tile_column, place, matrix_tiles, dual_bf,
        primal_start.reshape(COL_BLOCKS, 8, 128),
    )

    for iteration in range(ITERS):
        first, last = iteration == 0, iteration == ITERS - 1
        arrived = summed(own, other)
        send_shape = sds((CHIPS, SHARE, 128), f32 if last else bf16)
        if first:
            primal, send, change, weight, sigma, cost, upper = call(
                lambda *refs: update_kernel(True, *refs),
                "update",
                [VMEM, SMEM] + [VMEM] * 3,
                (part, send_shape, tiny, tiny, tiny, part, part),
                (VMEM,) * 7,
                limit=4,
            )(
                arrived, place, primal_start.reshape(wide), cost_vector.reshape(wide),
                upper_bound.reshape(wide),
            )
        else:
            primal, send, change, weight, sigma = call(
                lambda *refs: update_kernel(False, *refs),
                "update",
                [VMEM] * 5,
                (part, send_shape, tiny, tiny, tiny),
                (VMEM,) * 5,
                limit=4,
            )(arrived, primal, cost, upper, weight)
        near, far = gathered(send)
        if last:
            break
        dual, before, own, other = middle_call(
            tile_column, owners, place, matrix_tiles, kept, near, far, bounds, dual, before, change,
            sigma,
        )
    primal_final, send = last_call(
        tile_column, owners, place, destination, matrix_tiles, kept, near, far, bounds, dual, before, change,
        sigma,
    )
    same, cross = gathered(send)
    dual_final, weight = call(
        finish_kernel,
        "finish",
        [SMEM, VMEM, VMEM, VMEM],
        (sds((BLOCKS, TR)), sds((1,))),
        (VMEM, SMEM),
        limit=4,
    )(place, same, cross, weight)
    return (primal_final.reshape(-1), dual_final.reshape(-1), weight)


def solution(mesh):
    split = Mesh(
        mesh.devices.reshape(mesh.shape["grp"], 4, 4, 2), ("grp", "dev_0", "dev_1", "dev_2")
    )
    return jax.shard_map(
        per_device,
        mesh=split,
        in_specs=(
            P(ALL, None, None),
            P(ALL),
            P(ALL),
            P(ALL),
            P(ALL),
            P(ALL),
            P(),
            P(),
            P(),
        ),
        out_specs=(P(), P(ALL), P()),
        check_vma=False,
    )
```

```python
import jax
import jax.numpy as jnp
from jax import lax
from jax.experimental import pallas as pl
from jax.experimental.pallas import tpu as pltpu
from jax.sharding import Mesh
from jax.sharding import PartitionSpec as P

ITERS = 3
STEP = 0.3
TINY = 1e-06
BLOCKS = 32
MAXC = 4
AT_OWNER = 0
AT_COLUMN = 96
AT_TARGET = AT_COLUMN + 80
AT_PLACE = AT_TARGET + 32
INDEX = 256
SLOTS = 80
TR = 128
CB = 1024
COL_BLOCKS = 256
ROWS_P = 2048
CHIPS = 64
SHARE = 16
KEPT = 12
STOPS = (8, 12, 20, 28, 36, 44, 52, 60, 68, 76, 80)
STARTS = (0,) + STOPS[:-1]
CHUNKS = len(STOPS)

CHIP = ("grp", "dev_0", "dev_1")
CORE = "dev_2"
ALL = ("grp", "dev_0", "dev_1", "dev_2")
SWAP = [(0, 1), (1, 0)]
MIB = 1 << 20
PASS_LIMIT = 48

f32 = jnp.float32
bf16 = jnp.bfloat16


def round_bf16(x):
    return x.astype(bf16).astype(f32)


class View:
    def __init__(self, ref, base):
        self.ref, self.base = ref, base

    def __getitem__(self, i):
        return self.ref[self.base + i]


def views(index_ref):
    return tuple(View(index_ref, base) for base in (AT_COLUMN, AT_OWNER, AT_PLACE, AT_TARGET))


def fill_index(raw_ref, index_ref):
    for s in range(SLOTS):
        index_ref[AT_OWNER + s] = BLOCKS
    at = jnp.int32(AT_OWNER)
    for b in range(BLOCKS):
        for k in range(MAXC):
            index_ref[at + k] = b
        at = at + raw_ref[b]
    for k in range(MAXC):
        index_ref[at + k] = BLOCKS
    for i in range(SLOTS + BLOCKS + 3):
        index_ref[AT_COLUMN + i] = raw_ref[BLOCKS + i]


def row_tile(s, column_ref, tiles, table_ref, rough):
    col = column_ref[s]
    parts = [jnp.broadcast_to(table_ref[col, pl.ds(part, 1), :], (8, 128)) for part in range(8)]
    if rough:
        parts = [round_bf16(p) for p in parts]
    sums = []
    for g in range(TR // 8):
        rows = tiles[s, pl.ds(8 * g, 8), slice(None)].astype(f32)
        total = rows[:, 0:128] * parts[0]
        for part in range(1, 8):
            total = total + rows[:, 128 * part : 128 * part + 128] * parts[part]
        sums.append(total)
    return jnp.sum(jnp.concatenate(sums, axis=0).T.reshape(16, 8, 128), axis=0)


def row_chunk(i, arrive, column_ref, owner_ref, tiles, table_ref, image_ref, rough=False):
    arrive(i)
    results = [row_tile(s, column_ref, tiles, table_ref, rough) for s in chunk_of(i)]
    for s, r in zip(chunk_of(i), results):
        image_ref[owner_ref[s]] += r


def image_rows(image_ref):
    return jnp.concatenate(
        [jnp.sum(image_ref[b], axis=0, keepdims=True) for b in range(BLOCKS)], axis=0
    )


def column_tiles(slots, lefts, column_ref, tiles, sum_ref):
    sub = lax.broadcasted_iota(jnp.int32, (8, 128), 0)
    results = []
    for s, left in zip(slots, lefts):
        left = jnp.broadcast_to(left, (8, TR)).astype(bf16)
        out = jnp.dot(left, tiles[s], preferred_element_type=f32)
        r = out[:, 0:128]
        for part in range(1, 8):
            r = jnp.where(sub == part, out[:, 128 * part : 128 * part + 128], r)
        results.append(r)
    for s, r in zip(slots, results):
        sum_ref[column_ref[s]] += r


def clear_blocks(ref):
    n = ref.shape[0]

    def clear(i, carry):
        ref[i] = jnp.zeros((8, 128), f32)
        return carry

    lax.fori_loop(0, n, clear, 0, unroll=8 if n % 8 == 0 else 3)


def put_sums(sum_ref, core, own_ref, other_ref, scalars):
    def put(i, carry):
        for ref, side in ((own_ref, core), (other_ref, 1 - core)):
            at = side * (COL_BLOCKS // 2) + 2 * i
            ref[i, pl.ds(0, 8), :] = sum_ref[at]
            ref[i, pl.ds(8, 8), :] = sum_ref[at + 1]
            if scalars is not None:
                ref[i, pl.ds(SHARE, 8), :] = scalars
        return carry

    lax.fori_loop(0, CHIPS, put, 0, unroll=4)


def chunk_of(i):
    return range(STARTS[i], STOPS[i])


def start_tiles(tiles_hbm, kept_ref, tile_ref, sem, first):
    copies = {}
    for i in range(CHUNKS):
        start, size = STARTS[i], STOPS[i] - STARTS[i]
        if start < KEPT and not first:
            continue
        to, base = (kept_ref, 0) if start < KEPT else (tile_ref, KEPT)
        copies[i] = pltpu.make_async_copy(
            tiles_hbm.at[pl.ds(start, size)], to.at[pl.ds(start - base, size)], sem.at[i]
        )
        copies[i].start()

    def arrive(i):
        if i in copies:
            copies[i].wait()

    return arrive


class Tiles:
    def __init__(self, kept_ref, tile_ref):
        self.refs = kept_ref, tile_ref

    def __getitem__(self, at):
        s = at[0] if isinstance(at, tuple) else at
        rest = at[1:] if isinstance(at, tuple) else ()
        ref, base = (self.refs[0], 0) if s < KEPT else (self.refs[1], KEPT)
        return ref[(s - base, *rest)]


def first_kernel(
    raw_ref, tiles_hbm, dual_hbm, primal_hbm,
    index_ref, image_out, own_ref, other_ref, kept_ref,
    dual_ref, wide_ref, table_ref, tile_ref, sum_ref, image_ref,
    tile_sem, side_sem,
):
    sides = [
        pltpu.make_async_copy(src, dst, side_sem.at[i])
        for i, (src, dst) in enumerate(
            (
                (dual_hbm, dual_ref),
                (primal_hbm, table_ref),
            )
        )
    ]
    for copy in sides:
        copy.start()
    arrive = start_tiles(tiles_hbm, kept_ref, tile_ref, tile_sem, True)
    tiles = Tiles(kept_ref, tile_ref)
    clear_blocks(sum_ref)
    clear_blocks(image_ref)
    fill_index(raw_ref, index_ref)
    column_ref, owner_ref, place_ref, _ = views(index_ref)
    for copy in sides:
        copy.wait()
    wide_ref[pl.ds(0, BLOCKS), :] = dual_ref[...].astype(f32)
    wide_ref[pl.ds(BLOCKS, 8), :] = jnp.zeros((8, TR), f32)

    for i in range(CHUNKS):
        row_chunk(i, arrive, column_ref, owner_ref, tiles, table_ref, image_ref, True)
        lefts = [wide_ref[pl.ds(owner_ref[s], 1), :] for s in chunk_of(i)]
        column_tiles(chunk_of(i), lefts, column_ref, tiles, sum_ref)
    image_out[...] = image_rows(image_ref)
    put_sums(sum_ref, place_ref[0], own_ref, other_ref, None)


def merge_kernel(own_ref, other_ref, out_ref):
    rows = own_ref.shape[1]
    if rows > SHARE:
        rest = own_ref[0, pl.ds(SHARE, 8), :] + other_ref[0, pl.ds(SHARE, 8), :]
        sub = lax.broadcasted_iota(jnp.int32, (8, 128), 0)
        parts = jnp.zeros((8, 128), f32)
        for p in range(3):
            head = round_bf16(rest)
            parts = jnp.where(sub == p, head, parts)
            rest = rest - head
        parts = parts.astype(bf16)

    def add(i, carry):
        data = pl.ds(0, SHARE)
        out_ref[i, data, :] = (own_ref[i, data, :] + other_ref[i, data, :]).astype(bf16)
        if rows > SHARE:
            out_ref[i, pl.ds(SHARE, 8), :] = parts
        return carry

    lax.fori_loop(0, CHIPS, add, 0, unroll=8)


def fill_table(own_ref, other_ref, core, table_ref):
    def fill(i, carry):
        for ref, side in ((own_ref, core), (other_ref, 1 - core)):
            part = ref[i].astype(f32) if ref.dtype == bf16 else round_bf16(ref[i])
            at = side * (COL_BLOCKS // 2) + 2 * i
            table_ref[at] = part[0:8]
            table_ref[at + 1] = part[8:16]
        return carry

    lax.fori_loop(0, CHIPS, fill, 0, unroll=4)


def dual_step(bounds_ref, dual_in, image_before, image, change_in, sigma):
    bounds = bounds_ref[...]
    dual = jnp.maximum(
        dual_in[...] + sigma * (bounds - (2.0 * image - image_before)), 0.0
    )
    short = jnp.maximum(bounds - image, 0.0)
    violation = jnp.sum(short * short)
    lane = lax.broadcasted_iota(jnp.int32, (8, 128), 1)
    scalars = jnp.where(lane == 0, violation, jnp.where(lane == 1, change_in[...], 0.0))
    return dual, scalars


def middle_kernel(
    index_ref, tiles_hbm, kept_ref, own_in, other_in, bounds_ref, dual_in,
    before_ref, change_in, sigma_in,
    dual_ref, image_out, own_ref, other_ref,
    table_ref, tile_ref, sum_ref, image_ref, tile_sem,
):
    column_ref, owner_ref, place_ref, target_ref = views(index_ref)
    core = place_ref[0]
    arrive = start_tiles(tiles_hbm, kept_ref, tile_ref, tile_sem, False)
    tiles = Tiles(kept_ref, tile_ref)
    fill_table(own_in, other_in, core, table_ref)
    clear_blocks(sum_ref)
    clear_blocks(image_ref)
    sigma = sigma_in[0:1, :]

    def left(s):
        b = owner_ref[s]
        at = pl.ds(jnp.minimum(b, BLOCKS - 1), 1)
        image = jnp.sum(image_ref[b], axis=0, keepdims=True)
        move = bounds_ref[at, :] - (2.0 * image - before_ref[at, :])
        row = jnp.maximum(dual_in[at, :] + sigma * move, 0.0)
        return jnp.where(b < BLOCKS, row, 0.0)

    done = 0
    for i in range(CHUNKS):
        slots = range(done, max(STARTS[i] - 3, 0))
        lefts = [left(s) for s in slots]
        row_chunk(i, arrive, column_ref, owner_ref, tiles, table_ref, image_ref)
        column_tiles(slots, lefts, column_ref, tiles, sum_ref)
        done = slots.stop
    slots = range(done, SLOTS)
    lefts = [left(s) for s in slots]
    image = image_rows(image_ref)
    dual, scalars = dual_step(bounds_ref, dual_in, before_ref[...], image, change_in, sigma)
    image_out[...] = image
    dual_ref[...] = dual
    column_tiles(slots, lefts, column_ref, tiles, sum_ref)
    put_sums(sum_ref, core, own_ref, other_ref, scalars)


def last_kernel(
    index_ref, tiles_hbm, kept_ref, own_in, other_in, bounds_ref,
    dual_in, before_ref, change_in, sigma_in,
    primal_hbm, send_ref,
    table_ref, tile_ref, image_ref, tile_sem, out_sem,
):
    column_ref, owner_ref, place_ref, target_ref = views(index_ref)
    core = place_ref[0]
    arrive = start_tiles(tiles_hbm, kept_ref, tile_ref, tile_sem, False)
    tiles = Tiles(kept_ref, tile_ref)
    fill_table(own_in, other_in, core, table_ref)
    clear_blocks(image_ref)

    half = CHIPS
    outs = [
        pltpu.make_async_copy(ref, primal_hbm.at[pl.ds(side * half, half)], out_sem.at[i])
        for i, (ref, side) in enumerate(((own_in, core), (other_in, 1 - core)))
    ]
    for copy in outs:
        copy.start()
    for i in range(CHUNKS):
        row_chunk(i, arrive, column_ref, owner_ref, tiles, table_ref, image_ref)
    dual, scalars = dual_step(
        bounds_ref, dual_in, before_ref[...], image_rows(image_ref), change_in, sigma_in[0:1, :]
    )

    def put(i, carry):
        send_ref[i] = scalars
        return carry

    lax.fori_loop(0, CHIPS, put, 0, unroll=8)
    first = place_ref[2] * (BLOCKS // 2)
    for b in range(BLOCKS):
        to = target_ref[b]
        send_ref[first + jnp.right_shift(to, 1), pl.ds(jnp.bitwise_and(to, 1), 1), :] = dual[
            b : b + 1, :
        ]
    for copy in outs:
        copy.wait()


def next_weight(weight, scalars):
    lane = lax.broadcasted_iota(jnp.int32, (8, 128), 1)
    violation = jnp.sum(jnp.where(lane == 0, scalars, 0.0), axis=1, keepdims=True)
    change = jnp.sum(jnp.where(lane == 1, scalars, 0.0), axis=1, keepdims=True)
    ratio = jnp.broadcast_to((violation + TINY) / (change + TINY), (8, 128))
    return jnp.sqrt(weight * jnp.sqrt(ratio))


def update_kernel(first, *refs):
    if first:
        (arrived_ref, index_ref, primal_full, cost_full, upper_full,
         primal_ref, send_ref, change_ref, weight_ref, sigma_ref, cost_ref, upper_ref) = refs
        place_ref = views(index_ref)[2]
        at = pl.ds(pl.multiple_of(place_ref[1] * SHARE, SHARE), SHARE)
        primal, cost, upper = primal_full[at, :], cost_full[at, :], upper_full[at, :]
        cost_ref[...] = cost
        upper_ref[...] = upper
    else:
        (arrived_ref, primal_in, cost_in, upper_in, weight_in,
         send_ref, change_ref, weight_ref, sigma_ref, *primal_ref) = refs
        primal_ref = primal_ref[0] if primal_ref else None
        primal, cost, upper = primal_in[...], cost_in[...], upper_in[...]
    rows = arrived_ref.shape[1]

    def add(i, total):
        return total + arrived_ref[i].astype(f32)

    total = lax.fori_loop(0, CHIPS, add, jnp.zeros((rows, 128), f32), unroll=8)
    if first:
        weight = jnp.ones((8, 128), f32)
    else:
        scalars = total[SHARE : SHARE + 1, :] + total[SHARE + 1 : SHARE + 2, :]
        scalars = scalars + total[SHARE + 2 : SHARE + 3, :]
        weight = next_weight(weight_in[...], jnp.broadcast_to(scalars, (8, 128)))
    tau = STEP / weight[0:1, :]
    new = jnp.clip(primal - tau * (cost - total[:SHARE, :]), 0.0, upper)
    if primal_ref is not None:
        primal_ref[...] = new
    moved = new - primal
    change_ref[...] = jnp.full((8, 128), jnp.sum(moved * moved), f32)
    weight_ref[...] = weight
    sigma_ref[...] = STEP * weight
    out = new.astype(send_ref.dtype)

    def put(i, carry):
        send_ref[i] = out
        return carry

    lax.fori_loop(0, CHIPS, put, 0, unroll=8)


def finish_kernel(index_ref, same_ref, cross_ref, weight_in, dual_ref, weight_ref):
    def add(i, total):
        return total + (same_ref[i] + cross_ref[i])

    total = lax.fori_loop(0, CHIPS, add, jnp.zeros((8, 128), f32), unroll=8)
    total = jnp.broadcast_to(total[2:3, :], (8, 128))
    place_ref = views(index_ref)[2]
    weight_ref[0] = next_weight(weight_in[...], total)[0, 0]
    core = place_ref[0]
    first = place_ref[2] * (BLOCKS // 2)
    for chip in range(BLOCKS // 2):
        same = same_ref[first + chip, pl.ds(core, 1), :]
        cross = cross_ref[first + chip, pl.ds(core, 1), :]
        dual_ref[pl.ds(2 * chip + core, 1), :] = same
        dual_ref[pl.ds(2 * chip + 1 - core, 1), :] = cross


SMEM = pl.BlockSpec(memory_space=pltpu.SMEM)
VMEM = pl.BlockSpec(memory_space=pltpu.VMEM)
ANY = pl.BlockSpec(memory_space=pl.ANY)


def sds(shape, dtype=f32):
    return jax.ShapeDtypeStruct(shape, dtype)


def call(kernel, name, in_specs, out_shape, out_specs, scratch=(), limit=8):
    return pl.pallas_call(
        kernel,
        name=name,
        in_specs=in_specs,
        out_specs=out_specs,
        out_shape=out_shape,
        scratch_shapes=list(scratch),
        compiler_params=pltpu.CompilerParams(vmem_limit_bytes=limit * MIB),
    )


TILE = pltpu.VMEM((SLOTS - KEPT, TR, CB), bf16)
TABLE = pltpu.VMEM((COL_BLOCKS, 8, 128), f32)
IMAGE = pltpu.VMEM((BLOCKS + 1, 8, 128), f32)
DMA = pltpu.SemaphoreType.DMA


def first_call(*args):
    return call(
        first_kernel,
        "first_pass",
        [SMEM, ANY, ANY, ANY],
        (
            sds((INDEX,), jnp.int32),
            sds((BLOCKS, TR)),
            sds((CHIPS, SHARE, 128)),
            sds((CHIPS, SHARE, 128)),
            sds((KEPT, TR, CB), bf16),
        ),
        (SMEM, VMEM, VMEM, VMEM, VMEM),
        (
            pltpu.VMEM((BLOCKS, TR), bf16),
            pltpu.VMEM((BLOCKS + 8, TR), f32),
            TABLE,
            TILE,
            TABLE,
            IMAGE,
            DMA((CHUNKS,)),
            DMA((2,)),
        ),
        limit=PASS_LIMIT,
    )(*args)


def middle_call(*args):
    return call(
        middle_kernel,
        "middle_pass",
        [SMEM, ANY] + [VMEM] * 8,
        (sds((BLOCKS, TR)), sds((BLOCKS, TR))) + (sds((CHIPS, SHARE + 8, 128)),) * 2,
        (VMEM,) * 4,
        (TABLE, TILE, TABLE, IMAGE, DMA((CHUNKS,))),
        limit=PASS_LIMIT,
    )(*args)


def last_call(*args):
    return call(
        last_kernel,
        "last_pass",
        [SMEM, ANY] + [VMEM] * 8,
        (sds((2 * CHIPS, SHARE, 128)), sds((CHIPS, 8, 128))),
        (ANY, VMEM),
        (TABLE, TILE, IMAGE, DMA((CHUNKS,)), DMA((2,))),
        limit=PASS_LIMIT,
    )(*args)


def summed(own, other):
    crossed = lax.ppermute(other, CORE, SWAP)
    merged = call(merge_kernel, "merge", [VMEM] * 2, sds(own.shape, bf16), VMEM, limit=4)(
        own, crossed
    )
    return lax.all_to_all(merged, CHIP, 0, 0, tiled=True)


def gathered(send):
    own = lax.all_to_all(send, CHIP, 0, 0, tiled=True)
    return own, lax.ppermute(own, CORE, SWAP)


def per_device(
    matrix_tiles,
    tile_column,
    block_counts,
    destination,
    row_bounds,
    dual_start,
    primal_start,
    cost_vector,
    upper_bound,
):
    core = lax.axis_index(CORE)
    place = jnp.stack(
        [core, core * CHIPS + lax.axis_index(CHIP), lax.axis_index("grp")]
    ).astype(jnp.int32)
    raw = jnp.concatenate([block_counts, tile_column, destination, place])
    bounds = row_bounds.astype(f32).reshape(BLOCKS, TR)
    dual_bf = dual_start.reshape(BLOCKS, TR)
    dual = dual_bf.astype(f32)
    wide = (ROWS_P, 128)
    part = sds((SHARE, 128))
    tiny = sds((8, 128))

    index, before, own, other, kept = first_call(
        raw, matrix_tiles, dual_bf,
        primal_start.reshape(COL_BLOCKS, 8, 128),
    )

    for iteration in range(ITERS):
        first, last = iteration == 0, iteration == ITERS - 1
        arrived = summed(own, other)
        send_shape = sds((CHIPS, SHARE, 128), f32 if last else bf16)
        if first:
            primal, send, change, weight, sigma, cost, upper = call(
                lambda *refs: update_kernel(True, *refs),
                "update",
                [VMEM, SMEM] + [VMEM] * 3,
                (part, send_shape, tiny, tiny, tiny, part, part),
                (VMEM,) * 7,
                limit=4,
            )(
                arrived, index, primal_start.reshape(wide), cost_vector.reshape(wide),
                upper_bound.reshape(wide),
            )
        else:
            send, change, weight, sigma, *primal = call(
                lambda *refs: update_kernel(False, *refs),
                "update",
                [VMEM] * 5,
                (send_shape, tiny, tiny, tiny) + (() if last else (part,)),
                (VMEM,) * (4 if last else 5),
                limit=4,
            )(arrived, primal, cost, upper, weight)
            primal = None if last else primal[0]
        near, far = gathered(send)
        if last:
            break
        dual, before, own, other = middle_call(
            index, matrix_tiles, kept, near, far, bounds, dual, before, change,
            sigma,
        )
    primal_final, send = last_call(
        index, matrix_tiles, kept, near, far, bounds, dual, before, change,
        sigma,
    )
    same, cross = gathered(send)
    dual_final, weight = call(
        finish_kernel,
        "finish",
        [SMEM, VMEM, VMEM, VMEM],
        (sds((BLOCKS, TR)), sds((1,))),
        (VMEM, SMEM),
        limit=4,
    )(index, same, cross, weight)
    return (primal_final.reshape(-1), dual_final.reshape(-1), weight)


def solution(mesh):
    split = Mesh(
        mesh.devices.reshape(mesh.shape["grp"], 4, 4, 2), ("grp", "dev_0", "dev_1", "dev_2")
    )
    return jax.shard_map(
        per_device,
        mesh=split,
        in_specs=(
            P(ALL, None, None),
            P(ALL),
            P(ALL),
            P(ALL),
            P(ALL),
            P(ALL),
            P(),
            P(),
            P(),
        ),
        out_specs=(P(), P(ALL), P()),
        check_vma=False,
    )
```

```python
import jax
import jax.numpy as jnp
from jax import lax
from jax.experimental import pallas as pl
from jax.experimental.pallas import tpu as pltpu
from jax.sharding import Mesh
from jax.sharding import PartitionSpec as P

ITERS = 3
STEP = 0.3
TINY = 1e-06
BLOCKS = 32
MAXC = 4
AT_OWNER = 0
AT_COLUMN = 96
AT_TARGET = AT_COLUMN + 80
AT_PLACE = AT_TARGET + 32
INDEX = 256
SLOTS = 80
TR = 128
CB = 1024
COL_BLOCKS = 256
ROWS_P = 2048
CHIPS = 64
SHARE = 16
KEPT = 12
STOPS = (8, 12, 20, 28, 36, 44, 52, 60, 68, 76, 80)
STARTS = (0,) + STOPS[:-1]
CHUNKS = len(STOPS)

CHIP = ("grp", "dev_0", "dev_1")
CORE = "dev_2"
ALL = ("grp", "dev_0", "dev_1", "dev_2")
SWAP = [(0, 1), (1, 0)]
MIB = 1 << 20
PASS_LIMIT = 48

f32 = jnp.float32
bf16 = jnp.bfloat16


def round_bf16(x):
    return x.astype(bf16).astype(f32)


class View:
    def __init__(self, ref, base):
        self.ref, self.base = ref, base

    def __getitem__(self, i):
        return self.ref[self.base + i]


def views(index_ref):
    return tuple(View(index_ref, base) for base in (AT_COLUMN, AT_OWNER, AT_PLACE, AT_TARGET))


def fill_index(raw_ref, index_ref):
    for s in range(SLOTS):
        index_ref[AT_OWNER + s] = BLOCKS
    at = jnp.int32(AT_OWNER)
    for b in range(BLOCKS):
        for k in range(MAXC):
            index_ref[at + k] = b
        at = at + raw_ref[b]
    for k in range(MAXC):
        index_ref[at + k] = BLOCKS
    for i in range(SLOTS + BLOCKS + 3):
        index_ref[AT_COLUMN + i] = raw_ref[BLOCKS + i]


def row_tile(s, column_ref, tiles, table_ref, rough):
    col = column_ref[s]
    parts = [jnp.broadcast_to(table_ref[col, pl.ds(part, 1), :], (8, 128)) for part in range(8)]
    if rough:
        parts = [round_bf16(p) for p in parts]
    sums = []
    for g in range(TR // 8):
        rows = tiles[s, pl.ds(8 * g, 8), slice(None)].astype(f32)
        total = rows[:, 0:128] * parts[0]
        for part in range(1, 8):
            total = total + rows[:, 128 * part : 128 * part + 128] * parts[part]
        sums.append(total)
    return jnp.sum(jnp.concatenate(sums, axis=0).T.reshape(16, 8, 128), axis=0)


def row_chunk(i, arrive, column_ref, owner_ref, tiles, table_ref, image_ref, rough=False):
    arrive(i)
    results = [row_tile(s, column_ref, tiles, table_ref, rough) for s in chunk_of(i)]
    for s, r in zip(chunk_of(i), results):
        image_ref[owner_ref[s]] += r


def image_rows(image_ref):
    return jnp.concatenate(
        [jnp.sum(image_ref[b], axis=0, keepdims=True) for b in range(BLOCKS)], axis=0
    )


def column_tiles(slots, lefts, column_ref, tiles, sum_ref):
    sub = lax.broadcasted_iota(jnp.int32, (8, 128), 0)
    results = []
    for s, left in zip(slots, lefts):
        left = jnp.broadcast_to(left, (8, TR)).astype(bf16)
        out = jnp.dot(left, tiles[s], preferred_element_type=f32)
        r = out[:, 0:128]
        for part in range(1, 8):
            r = jnp.where(sub == part, out[:, 128 * part : 128 * part + 128], r)
        results.append(r)
    for s, r in zip(slots, results):
        sum_ref[column_ref[s]] += r


def clear_blocks(ref):
    n = ref.shape[0]

    def clear(i, carry):
        ref[i] = jnp.zeros((8, 128), f32)
        return carry

    lax.fori_loop(0, n, clear, 0, unroll=8 if n % 8 == 0 else 3)


def put_sums(sum_ref, core, own_ref, other_ref, scalars):
    def put(i, carry):
        for ref, side in ((own_ref, core), (other_ref, 1 - core)):
            at = side * (COL_BLOCKS // 2) + 2 * i
            ref[i, pl.ds(0, 8), :] = sum_ref[at]
            ref[i, pl.ds(8, 8), :] = sum_ref[at + 1]
        return carry

    lax.fori_loop(0, CHIPS, put, 0, unroll=4)
    if scalars is not None:
        for ref in (own_ref, other_ref):
            ref[CHIPS, pl.ds(0, 8), :] = scalars
            ref[CHIPS, pl.ds(8, 8), :] = scalars


def chunk_of(i):
    return range(STARTS[i], STOPS[i])


def start_tiles(tiles_hbm, kept_ref, tile_ref, sem, first):
    copies = {}
    for i in range(CHUNKS):
        start, size = STARTS[i], STOPS[i] - STARTS[i]
        if start < KEPT and not first:
            continue
        to, base = (kept_ref, 0) if start < KEPT else (tile_ref, KEPT)
        copies[i] = pltpu.make_async_copy(
            tiles_hbm.at[pl.ds(start, size)], to.at[pl.ds(start - base, size)], sem.at[i]
        )
        copies[i].start()

    def arrive(i):
        if i in copies:
            copies[i].wait()

    return arrive


class Tiles:
    def __init__(self, kept_ref, tile_ref):
        self.refs = kept_ref, tile_ref

    def __getitem__(self, at):
        s = at[0] if isinstance(at, tuple) else at
        rest = at[1:] if isinstance(at, tuple) else ()
        ref, base = (self.refs[0], 0) if s < KEPT else (self.refs[1], KEPT)
        return ref[(s - base, *rest)]


def first_kernel(
    raw_ref, tiles_hbm, dual_hbm, primal_hbm,
    index_ref, image_out, own_ref, other_ref, kept_ref,
    dual_ref, wide_ref, table_ref, tile_ref, sum_ref, image_ref,
    tile_sem, side_sem,
):
    sides = [
        pltpu.make_async_copy(src, dst, side_sem.at[i])
        for i, (src, dst) in enumerate(
            (
                (dual_hbm, dual_ref),
                (primal_hbm, table_ref),
            )
        )
    ]
    for copy in sides:
        copy.start()
    arrive = start_tiles(tiles_hbm, kept_ref, tile_ref, tile_sem, True)
    tiles = Tiles(kept_ref, tile_ref)
    clear_blocks(sum_ref)
    clear_blocks(image_ref)
    fill_index(raw_ref, index_ref)
    column_ref, owner_ref, place_ref, _ = views(index_ref)
    for copy in sides:
        copy.wait()
    wide_ref[pl.ds(0, BLOCKS), :] = dual_ref[...].astype(f32)
    wide_ref[pl.ds(BLOCKS, 8), :] = jnp.zeros((8, TR), f32)

    for i in range(CHUNKS):
        row_chunk(i, arrive, column_ref, owner_ref, tiles, table_ref, image_ref, True)
        lefts = [wide_ref[pl.ds(owner_ref[s], 1), :] for s in chunk_of(i)]
        column_tiles(chunk_of(i), lefts, column_ref, tiles, sum_ref)
    image_out[...] = image_rows(image_ref)
    put_sums(sum_ref, place_ref[0], own_ref, other_ref, None)


def merge_kernel(own_ref, other_ref, out_ref):
    rows = out_ref.shape[1]
    if rows > SHARE:
        rest = own_ref[CHIPS, pl.ds(0, 8), :] + other_ref[CHIPS, pl.ds(0, 8), :]
        sub = lax.broadcasted_iota(jnp.int32, (8, 128), 0)
        parts = jnp.zeros((8, 128), f32)
        for p in range(3):
            head = round_bf16(rest)
            parts = jnp.where(sub == p, head, parts)
            rest = rest - head
        parts = parts.astype(bf16)

    def add(i, carry):
        data = pl.ds(0, SHARE)
        out_ref[i, data, :] = (own_ref[i, data, :] + other_ref[i, data, :]).astype(bf16)
        if rows > SHARE:
            out_ref[i, pl.ds(SHARE, 8), :] = parts
        return carry

    lax.fori_loop(0, CHIPS, add, 0, unroll=8)


def fill_table(own_ref, other_ref, core, table_ref):
    def fill(i, carry):
        for ref, side in ((own_ref, core), (other_ref, 1 - core)):
            part = ref[i].astype(f32) if ref.dtype == bf16 else round_bf16(ref[i])
            at = side * (COL_BLOCKS // 2) + 2 * i
            table_ref[at] = part[0:8]
            table_ref[at + 1] = part[8:16]
        return carry

    lax.fori_loop(0, CHIPS, fill, 0, unroll=4)


def dual_step(bounds_ref, dual_in, image_before, image, change_in, sigma):
    bounds = bounds_ref[...]
    dual = jnp.maximum(
        dual_in[...] + sigma * (bounds - (2.0 * image - image_before)), 0.0
    )
    short = jnp.maximum(bounds - image, 0.0)
    violation = jnp.sum(short * short)
    lane = lax.broadcasted_iota(jnp.int32, (8, 128), 1)
    scalars = jnp.where(lane == 0, violation, jnp.where(lane == 1, change_in[...], 0.0))
    return dual, scalars


def middle_kernel(
    index_ref, tiles_hbm, kept_ref, own_in, other_in, bounds_ref, dual_in,
    before_ref, change_in, sigma_in,
    dual_ref, image_out, own_ref, other_ref,
    table_ref, tile_ref, sum_ref, image_ref, tile_sem,
):
    column_ref, owner_ref, place_ref, target_ref = views(index_ref)
    core = place_ref[0]
    arrive = start_tiles(tiles_hbm, kept_ref, tile_ref, tile_sem, False)
    tiles = Tiles(kept_ref, tile_ref)
    fill_table(own_in, other_in, core, table_ref)
    clear_blocks(sum_ref)
    clear_blocks(image_ref)
    sigma = sigma_in[0:1, :]

    def left(s):
        b = owner_ref[s]
        at = pl.ds(jnp.minimum(b, BLOCKS - 1), 1)
        image = jnp.sum(image_ref[b], axis=0, keepdims=True)
        move = bounds_ref[at, :] - (2.0 * image - before_ref[at, :])
        row = jnp.maximum(dual_in[at, :] + sigma * move, 0.0)
        return jnp.where(b < BLOCKS, row, 0.0)

    done = 0
    for i in range(CHUNKS):
        slots = range(done, max(STARTS[i] - 3, 0))
        lefts = [left(s) for s in slots]
        row_chunk(i, arrive, column_ref, owner_ref, tiles, table_ref, image_ref)
        column_tiles(slots, lefts, column_ref, tiles, sum_ref)
        done = slots.stop
    slots = range(done, SLOTS)
    lefts = [left(s) for s in slots]
    image = image_rows(image_ref)
    dual, scalars = dual_step(bounds_ref, dual_in, before_ref[...], image, change_in, sigma)
    image_out[...] = image
    dual_ref[...] = dual
    column_tiles(slots, lefts, column_ref, tiles, sum_ref)
    put_sums(sum_ref, core, own_ref, other_ref, scalars)


def last_kernel(
    index_ref, tiles_hbm, kept_ref, own_in, other_in, bounds_ref,
    dual_in, before_ref, change_in, sigma_in,
    primal_hbm, send_ref,
    table_ref, tile_ref, image_ref, tile_sem, out_sem,
):
    column_ref, owner_ref, place_ref, target_ref = views(index_ref)
    core = place_ref[0]
    arrive = start_tiles(tiles_hbm, kept_ref, tile_ref, tile_sem, False)
    tiles = Tiles(kept_ref, tile_ref)
    fill_table(own_in, other_in, core, table_ref)
    clear_blocks(image_ref)

    half = CHIPS
    outs = [
        pltpu.make_async_copy(ref, primal_hbm.at[pl.ds(side * half, half)], out_sem.at[i])
        for i, (ref, side) in enumerate(((own_in, core), (other_in, 1 - core)))
    ]
    for copy in outs:
        copy.start()
    for i in range(CHUNKS):
        row_chunk(i, arrive, column_ref, owner_ref, tiles, table_ref, image_ref)
    dual, scalars = dual_step(
        bounds_ref, dual_in, before_ref[...], image_rows(image_ref), change_in, sigma_in[0:1, :]
    )

    def put(i, carry):
        send_ref[i] = scalars
        return carry

    lax.fori_loop(0, CHIPS, put, 0, unroll=8)
    first = place_ref[2] * (BLOCKS // 2)
    for b in range(BLOCKS):
        to = target_ref[b]
        send_ref[first + jnp.right_shift(to, 1), pl.ds(jnp.bitwise_and(to, 1), 1), :] = dual[
            b : b + 1, :
        ]
    for copy in outs:
        copy.wait()


def next_weight(weight, scalars):
    lane = lax.broadcasted_iota(jnp.int32, (8, 128), 1)
    violation = jnp.sum(jnp.where(lane == 0, scalars, 0.0), axis=1, keepdims=True)
    change = jnp.sum(jnp.where(lane == 1, scalars, 0.0), axis=1, keepdims=True)
    ratio = jnp.broadcast_to((violation + TINY) / (change + TINY), (8, 128))
    return jnp.sqrt(weight * jnp.sqrt(ratio))


def update_kernel(first, *refs):
    if first:
        (arrived_ref, index_ref, primal_full, cost_full, upper_full,
         primal_ref, send_ref, change_ref, weight_ref, sigma_ref, cost_ref, upper_ref) = refs
        place_ref = views(index_ref)[2]
        at = pl.ds(pl.multiple_of(place_ref[1] * SHARE, SHARE), SHARE)
        primal, cost, upper = primal_full[at, :], cost_full[at, :], upper_full[at, :]
        cost_ref[...] = cost
        upper_ref[...] = upper
    else:
        (arrived_ref, primal_in, cost_in, upper_in, weight_in,
         send_ref, change_ref, weight_ref, sigma_ref, *primal_ref) = refs
        primal_ref = primal_ref[0] if primal_ref else None
        primal, cost, upper = primal_in[...], cost_in[...], upper_in[...]
    rows = arrived_ref.shape[1]

    def add(i, total):
        return total + arrived_ref[i].astype(f32)

    total = lax.fori_loop(0, CHIPS, add, jnp.zeros((rows, 128), f32), unroll=8)
    if first:
        weight = jnp.ones((8, 128), f32)
    else:
        scalars = total[SHARE : SHARE + 1, :] + total[SHARE + 1 : SHARE + 2, :]
        scalars = scalars + total[SHARE + 2 : SHARE + 3, :]
        weight = next_weight(weight_in[...], jnp.broadcast_to(scalars, (8, 128)))
    tau = STEP / weight[0:1, :]
    new = jnp.clip(primal - tau * (cost - total[:SHARE, :]), 0.0, upper)
    if primal_ref is not None:
        primal_ref[...] = new
    moved = new - primal
    change_ref[...] = jnp.full((8, 128), jnp.sum(moved * moved), f32)
    weight_ref[...] = weight
    sigma_ref[...] = STEP * weight
    out = new.astype(send_ref.dtype)

    def put(i, carry):
        send_ref[i] = out
        return carry

    lax.fori_loop(0, CHIPS, put, 0, unroll=8)


def finish_kernel(index_ref, same_ref, cross_ref, weight_in, dual_ref, weight_ref):
    def add(i, total):
        return total + (same_ref[i] + cross_ref[i])

    total = lax.fori_loop(0, CHIPS, add, jnp.zeros((8, 128), f32), unroll=8)
    total = jnp.broadcast_to(total[2:3, :], (8, 128))
    place_ref = views(index_ref)[2]
    weight_ref[0] = next_weight(weight_in[...], total)[0, 0]
    core = place_ref[0]
    first = place_ref[2] * (BLOCKS // 2)
    for chip in range(BLOCKS // 2):
        same = same_ref[first + chip, pl.ds(core, 1), :]
        cross = cross_ref[first + chip, pl.ds(core, 1), :]
        dual_ref[pl.ds(2 * chip + core, 1), :] = same
        dual_ref[pl.ds(2 * chip + 1 - core, 1), :] = cross


SMEM = pl.BlockSpec(memory_space=pltpu.SMEM)
VMEM = pl.BlockSpec(memory_space=pltpu.VMEM)
ANY = pl.BlockSpec(memory_space=pl.ANY)


def sds(shape, dtype=f32):
    return jax.ShapeDtypeStruct(shape, dtype)


def call(kernel, name, in_specs, out_shape, out_specs, scratch=(), limit=8):
    return pl.pallas_call(
        kernel,
        name=name,
        in_specs=in_specs,
        out_specs=out_specs,
        out_shape=out_shape,
        scratch_shapes=list(scratch),
        compiler_params=pltpu.CompilerParams(vmem_limit_bytes=limit * MIB),
    )


TILE = pltpu.VMEM((SLOTS - KEPT, TR, CB), bf16)
TABLE = pltpu.VMEM((COL_BLOCKS, 8, 128), f32)
IMAGE = pltpu.VMEM((BLOCKS + 1, 8, 128), f32)
DMA = pltpu.SemaphoreType.DMA


def first_call(*args):
    return call(
        first_kernel,
        "first_pass",
        [SMEM, ANY, ANY, ANY],
        (
            sds((INDEX,), jnp.int32),
            sds((BLOCKS, TR)),
            sds((CHIPS, SHARE, 128)),
            sds((CHIPS, SHARE, 128)),
            sds((KEPT, TR, CB), bf16),
        ),
        (SMEM, VMEM, VMEM, VMEM, VMEM),
        (
            pltpu.VMEM((BLOCKS, TR), bf16),
            pltpu.VMEM((BLOCKS + 8, TR), f32),
            TABLE,
            TILE,
            TABLE,
            IMAGE,
            DMA((CHUNKS,)),
            DMA((2,)),
        ),
        limit=PASS_LIMIT,
    )(*args)


def middle_call(*args):
    return call(
        middle_kernel,
        "middle_pass",
        [SMEM, ANY] + [VMEM] * 8,
        (sds((BLOCKS, TR)), sds((BLOCKS, TR))) + (sds((CHIPS + 1, SHARE, 128)),) * 2,
        (VMEM,) * 4,
        (TABLE, TILE, TABLE, IMAGE, DMA((CHUNKS,))),
        limit=PASS_LIMIT,
    )(*args)


def last_call(*args):
    return call(
        last_kernel,
        "last_pass",
        [SMEM, ANY] + [VMEM] * 8,
        (sds((2 * CHIPS, SHARE, 128)), sds((CHIPS, 8, 128))),
        (ANY, VMEM),
        (TABLE, TILE, IMAGE, DMA((CHUNKS,)), DMA((2,))),
        limit=PASS_LIMIT,
    )(*args)


def summed(own, other):
    crossed = lax.ppermute(other, CORE, SWAP)
    rows = SHARE if own.shape[0] == CHIPS else SHARE + 8
    merged = call(
        merge_kernel, "merge", [VMEM] * 2, sds((CHIPS, rows, 128), bf16), VMEM, limit=4
    )(own, crossed)
    return lax.all_to_all(merged, CHIP, 0, 0, tiled=True)


def gathered(send):
    own = lax.all_to_all(send, CHIP, 0, 0, tiled=True)
    return own, lax.ppermute(own, CORE, SWAP)


def per_device(
    matrix_tiles,
    tile_column,
    block_counts,
    destination,
    row_bounds,
    dual_start,
    primal_start,
    cost_vector,
    upper_bound,
):
    core = lax.axis_index(CORE)
    place = jnp.stack(
        [core, core * CHIPS + lax.axis_index(CHIP), lax.axis_index("grp")]
    ).astype(jnp.int32)
    raw = jnp.concatenate([block_counts, tile_column, destination, place])
    bounds = row_bounds.astype(f32).reshape(BLOCKS, TR)
    dual_bf = dual_start.reshape(BLOCKS, TR)
    dual = dual_bf.astype(f32)
    wide = (ROWS_P, 128)
    part = sds((SHARE, 128))
    tiny = sds((8, 128))

    index, before, own, other, kept = first_call(
        raw, matrix_tiles, dual_bf,
        primal_start.reshape(COL_BLOCKS, 8, 128),
    )

    for iteration in range(ITERS):
        first, last = iteration == 0, iteration == ITERS - 1
        arrived = summed(own, other)
        send_shape = sds((CHIPS, SHARE, 128), f32 if last else bf16)
        if first:
            primal, send, change, weight, sigma, cost, upper = call(
                lambda *refs: update_kernel(True, *refs),
                "update",
                [VMEM, SMEM] + [VMEM] * 3,
                (part, send_shape, tiny, tiny, tiny, part, part),
                (VMEM,) * 7,
                limit=4,
            )(
                arrived, index, primal_start.reshape(wide), cost_vector.reshape(wide),
                upper_bound.reshape(wide),
            )
        else:
            send, change, weight, sigma, *primal = call(
                lambda *refs: update_kernel(False, *refs),
                "update",
                [VMEM] * 5,
                (send_shape, tiny, tiny, tiny) + (() if last else (part,)),
                (VMEM,) * (4 if last else 5),
                limit=4,
            )(arrived, primal, cost, upper, weight)
            primal = None if last else primal[0]
        near, far = gathered(send)
        if last:
            break
        dual, before, own, other = middle_call(
            index, matrix_tiles, kept, near, far, bounds, dual, before, change,
            sigma,
        )
    primal_final, send = last_call(
        index, matrix_tiles, kept, near, far, bounds, dual, before, change,
        sigma,
    )
    same, cross = gathered(send)
    dual_final, weight = call(
        finish_kernel,
        "finish",
        [SMEM, VMEM, VMEM, VMEM],
        (sds((BLOCKS, TR)), sds((1,))),
        (VMEM, SMEM),
        limit=4,
    )(index, same, cross, weight)
    return (primal_final.reshape(-1), dual_final.reshape(-1), weight)


def solution(mesh):
    split = Mesh(
        mesh.devices.reshape(mesh.shape["grp"], 4, 4, 2), ("grp", "dev_0", "dev_1", "dev_2")
    )
    return jax.shard_map(
        per_device,
        mesh=split,
        in_specs=(
            P(ALL, None, None),
            P(ALL),
            P(ALL),
            P(ALL),
            P(ALL),
            P(ALL),
            P(),
            P(),
            P(),
        ),
        out_specs=(P(), P(ALL), P()),
        check_vma=False,
    )
```
